32 devices in a mesh: grp: 2 (over x), dap: 4 (over y, core), sub: 4 (over z).
Axes of the slice: x: 2, y: 2, z: 4, core: 2. Of those that a mesh axis runs over, the one named last changes fastest.
Arguments:
- alignment: bfloat16 [32, 16, 256], P(('grp', 'dap', 'sub')), parts along dimension 0, may hold values from -170 to 170
- pair_bias: bfloat16 [8, 32, 16], P(None, ('grp', 'dap', 'sub')), parts along dimension 1, may hold values from -4 to 250
- row_project: bfloat16 [256, 4, 256], replicated, may hold values from -0.375 to 0.375
- row_output: bfloat16 [256, 256], replicated, may hold values from -0.375 to 0.375
- column_project: bfloat16 [256, 4, 256], replicated, may hold values from -9 to 9
- column_output: bfloat16 [256, 256], replicated, may hold values from -0.375 to 0.375
- transition_in: bfloat16 [256, 2, 1024], replicated, may hold values from -0.375 to 0.375
- transition_out: bfloat16 [1024, 256], replicated, may hold values from -0.1875 to 0.1875
- cotangent: bfloat16 [32, 16, 256], P(('grp', 'dap', 'sub')), parts along dimension 0, may hold values from -6 to 6
Outputs:
- grad_alignment: bfloat16 [32, 16, 256], P(('grp', 'dap', 'sub')), parts along dimension 0
- grad_bias: float32 [8, 32, 16], P(None, ('grp', 'dap', 'sub')), parts along dimension 1
- grad_row_project: float32 [512, 4, 256], P(('grp', 'dap', 'sub')), parts along dimension 0
- grad_row_output: float32 [512, 256], P(('grp', 'dap', 'sub')), parts along dimension 0
- grad_column_project: float32 [512, 4, 256], P(('grp', 'dap', 'sub')), parts along dimension 0
- grad_column_output: float32 [512, 256], P(('grp', 'dap', 'sub')), parts along dimension 0
- grad_transition_in: float32 [512, 2, 1024], P(('grp', 'dap', 'sub')), parts along dimension 0
- grad_transition_out: float32 [2048, 256], P(('grp', 'dap', 'sub')), parts along dimension 0
The draws below stay inside these ranges and needn't reach their ends.
There are 2 independent parts, one for each index of `grp`. The reference program is written for one: setup_inputs(seed, part) draws one part's arguments, and reference() takes and returns one part's arrays. A program takes and returns all parts, laid end to end along the dimension named above; an argument that names none is the same for every part. Nothing has to cross between parts.
All inputs are finite; a program needn't handle non-finite values.
Results may differ from the reference program's by a relative error of at most 0.019.
Values may be sent and summed in bfloat16 or wider, within the bound.
No kernel may reach another device: no remote copies, remote signals or barrier semaphores. Data moves between devices by JAX's collectives and lax.ppermute only.
A program may use at most 64 MiB of HBM per device.

```python
import jax
import jax.numpy as jnp
from jax import lax

C = 256
H = 8
DH = 32
FF = 1024
S = 16
R = 16


def draw_alignment(key, part):
    sample = jnp.clip(jax.random.normal(jax.random.fold_in(key, 11), (S, R, C), jnp.float32), -5.0, 5.0)
    return sample.astype(jnp.bfloat16)


def draw_pair_bias(key, part):
    sample = jnp.clip(jax.random.normal(jax.random.fold_in(key, 21), (H, R, R), jnp.float32), -4.0, 4.0)
    return sample.astype(jnp.bfloat16)


def draw_column_project(key, part):
    sample = jnp.clip(jax.random.normal(jax.random.fold_in(key, 31), (C, 4, H * DH), jnp.float32), -6.0, 6.0) * C ** (-0.5)
    return sample.astype(jnp.bfloat16)


def spiked(result, rng, source, target, shards_of, factor):
    owner, partner = [(jnp.arange(result.shape[axis_at]) // (result.shape[axis_at] // shards_of)).reshape([-1 if axis == axis_at else 1 for axis in range(result.ndim)]) for axis_at in (source, target)]
    chosen = jax.random.permutation(rng, shards_of)[partner]
    strong = (owner == chosen) | (owner == (partner + shards_of // 2) % shards_of)
    return jnp.where(strong, factor * result, result)


def level_of(stream_key, shape, cuts, low, largest):
    def one(dim, parts):
        draws = jax.random.uniform(jax.random.fold_in(jax.random.fold_in(stream_key, 6), dim), (parts,), jnp.float32, low / len(cuts), largest / len(cuts))
        return jnp.repeat(jnp.exp(draws), shape[dim] // parts).reshape((-1,) + (1,) * (len(shape) - dim - 1))

    loudness = one(*cuts[0])
    for cut in cuts[1:]:
        loudness = loudness * one(*cut)
    return loudness


def gaussian(own_key, dims, deviation, reach, cuts=(), kind=jnp.bfloat16):
    drawn = jax.random.normal(own_key, dims, jnp.float32) * deviation
    if len(cuts) > 0:
        drawn = level_of(own_key, dims, cuts, -0.22, 0.18) * drawn
    return jnp.clip(drawn, min=-reach, max=reach).astype(kind)


def bell_draw_with(own_key, shape, scale, limit, split, heavy, held_as=jnp.bfloat16):
    entries = scale * jax.random.normal(own_key, shape, jnp.float32)
    if split:
        entries = entries * level_of(own_key, shape, split, -0.22, 0.18)
    return jnp.clip(spiked(entries, jax.random.fold_in(own_key, 3), *heavy), -limit, limit).astype(held_as)


def setup_inputs(seed: int = 0, part: int = 0) -> dict:
    seeds = jax.random.split(jax.random.key(seed), 10)
    part_splits = jax.random.split(jax.random.fold_in(seeds[9], part), 10)
    alignment = draw_alignment(jax.random.fold_in(jax.random.fold_in(seeds[9], part), 71), part)
    pair_bias = draw_pair_bias(jax.random.fold_in(jax.random.fold_in(seeds[9], part), 71), part)
    row_project = gaussian(seeds[2], (C, 4, H * DH), C ** -0.5, 0.375)
    row_output = gaussian(seeds[3], (H * DH, C), (H * DH) ** -0.5, 0.375)
    column_project = draw_column_project(jax.random.fold_in(seeds[9], 71), part)
    column_output = gaussian(seeds[5], (H * DH, C), (H * DH) ** -0.5, 0.375)
    transition_in = gaussian(seeds[6], (C, 2, FF), C ** -0.5, 0.375)
    transition_out = gaussian(seeds[7], (FF, C), FF ** -0.5, 0.1875)
    cotangent = bell_draw_with(part_splits[8], (S, R, C), 1.0, 6.0, ((0, 16),), (0, 1, 16, 2.0))
    return dict(alignment=alignment, pair_bias=pair_bias, row_project=row_project, row_output=row_output, column_project=column_project, column_output=column_output, transition_in=transition_in, transition_out=transition_out, cotangent=cotangent)


EPSILON = 1e-05

def product(pattern, former, latter):
    return jnp.einsum(pattern, former.astype(jnp.float32), latter.astype(jnp.float32))

def normalize(values):
    values = values.astype(jnp.float32)
    centred = values - lax.optimization_barrier(jnp.mean(values, axis=-1, keepdims=True))
    factor = lax.rsqrt(lax.optimization_barrier(jnp.mean(centred * centred, axis=-1, keepdims=True)) + EPSILON)
    return (centred * factor, factor)

def norm_back(normed, factor, upstream):
    mean_up = lax.optimization_barrier(jnp.mean(upstream, axis=-1, keepdims=True))
    mean_cross = lax.optimization_barrier(jnp.mean(upstream * normed, axis=-1, keepdims=True))
    return factor * (upstream - mean_up - normed * mean_cross)

def run_items(function, arrays, sequential):
    if sequential:
        return lax.map(lambda bundle: function(*bundle), arrays)
    return jax.vmap(function)(*arrays)

def head_shares(queries, key_rows, bias_head):
    scores = product('qd,kd->qk', queries, key_rows)
    if bias_head is not None:
        scores = scores + bias_head.astype(jnp.float32)
    row_top = lax.optimization_barrier(jnp.max(scores, axis=-1, keepdims=True))
    powered = jnp.exp(scores - row_top)
    return powered / lax.optimization_barrier(jnp.sum(powered, axis=-1, keepdims=True))

def head_forward(queries, key_rows, values, bias_head=None):
    shares = head_shares(queries, key_rows, bias_head)
    return product('qk,kd->qd', shares.astype(jnp.bfloat16), values)

def head_backward(queries, key_rows, values, grad_blend, bias_head=None):
    shares = head_shares(queries, key_rows, bias_head)
    shares_low = shares.astype(jnp.bfloat16)
    blended = product('qk,kd->qd', shares_low, values)
    grad_shares = product('qd,kd->qk', grad_blend, values)
    grad_values = product('qk,qd->kd', shares_low, grad_blend)
    centre = lax.optimization_barrier(jnp.sum(shares * grad_shares, axis=-1, keepdims=True))
    grad_scores = shares * (grad_shares - centre)
    grad_low = grad_scores.astype(jnp.bfloat16)
    grad_queries = product('qk,kd->qd', grad_low, key_rows)
    grad_keys = product('qk,qd->kd', grad_low, queries)
    return (blended, grad_queries, grad_keys, grad_values, grad_scores)

def item_project(normed_item, weights):
    projected = product('lc,cfhd->fhld', normed_item, weights.reshape(C, 4, H, DH))
    queries = (projected[0] * DH ** (-0.5)).astype(jnp.bfloat16)
    key_rows = projected[1].astype(jnp.bfloat16)
    values = projected[2].astype(jnp.bfloat16)
    gating = jax.nn.sigmoid(projected[3])
    return (queries, key_rows, values, gating)

def forward_item(normed_item, weights, bias_table, head_loop):
    queries, key_rows, values, gating = item_project(normed_item, weights)
    if bias_table is None:
        head_args = (queries, key_rows, values)
    else:
        head_args = (queries, key_rows, values, bias_table)
    blended = run_items(head_forward, head_args, head_loop)
    return (blended * gating).astype(jnp.bfloat16)

def backward_item(normed_item, upstream_item, weights, out_weight, bias_table, head_loop):
    queries, key_rows, values, gating = item_project(normed_item, weights)
    grad_gated = product('lc,hdc->hld', upstream_item, out_weight.reshape(H, DH, C))
    grad_blend = (grad_gated * gating).astype(jnp.bfloat16)
    if bias_table is None:
        head_args = (queries, key_rows, values, grad_blend)
    else:
        head_args = (queries, key_rows, values, grad_blend, bias_table)
    blended, grad_queries, grad_keys, grad_values, grad_scores = run_items(head_backward, head_args, head_loop)
    grad_gate = grad_gated * blended * gating * (1.0 - gating)
    grad_proj = jnp.stack([grad_queries * DH ** (-0.5), grad_keys, grad_values, grad_gate], axis=0).astype(jnp.bfloat16)
    if bias_table is None:
        return (grad_proj, jnp.zeros((), jnp.float32))
    return (grad_proj, grad_scores)

def section_forward(normed_low, weights, bias_table, item_loop, head_loop):

    def single(normed_item):
        return forward_item(normed_item, weights, bias_table, head_loop)
    return run_items(single, (normed_low,), item_loop)

def section_backward(normed_low, upstream_low, weights, out_weight, bias_table, item_loop, head_loop):

    def single(normed_item, upstream_item):
        return backward_item(normed_item, upstream_item, weights, out_weight, bias_table, head_loop)
    if bias_table is None:
        grad_proj, unused = run_items(single, (normed_low, upstream_low), item_loop)
        return (grad_proj, None)

    def accumulate(running, bundle):
        grad_proj, grad_scores = single(bundle[0], bundle[1])
        return (running + grad_scores, grad_proj)
    bias_total, grad_proj = lax.scan(accumulate, jnp.zeros(bias_table.shape, jnp.float32), (normed_low, upstream_low))
    return (grad_proj, bias_total)

def column_block(columns, upstream, column_project, column_output, transition_in, transition_out, item_loop, head_loop):
    normed_cols, scale_cols = normalize(columns)
    normed_cols_low = normed_cols.astype(jnp.bfloat16)
    column_gated = section_forward(normed_cols_low, column_project, None, item_loop, head_loop)
    column_update = product('bhld,hdc->blc', column_gated, column_output.reshape(H, DH, C))
    after_columns = (columns.astype(jnp.float32) + column_update).astype(jnp.bfloat16)
    normed_two, scale_two = normalize(after_columns)
    normed_two_low = normed_two.astype(jnp.bfloat16)
    pre_hidden = product('blc,cfe->blfe', normed_two_low, transition_in)
    gate_part = pre_hidden[:, :, 0]
    up_part = pre_hidden[:, :, 1]
    sigmoid_gate = jax.nn.sigmoid(gate_part)
    activated = gate_part * sigmoid_gate
    hidden = (activated * up_part).astype(jnp.bfloat16)
    raw_trans_out = product('blf,blc->fc', hidden, upstream)
    grad_hidden = product('blc,fc->blf', upstream, transition_out)
    grad_gate_part = grad_hidden * up_part * sigmoid_gate * (1.0 + gate_part * (1.0 - sigmoid_gate))
    grad_up_part = grad_hidden * activated
    grad_pre = jnp.stack([grad_gate_part, grad_up_part], axis=2).astype(jnp.bfloat16)
    raw_trans_in = product('blc,blfe->cfe', normed_two_low, grad_pre)
    grad_normed_two = product('blfe,cfe->blc', grad_pre, transition_in)
    grad_after_columns = upstream.astype(jnp.float32) + norm_back(normed_two, scale_two, grad_normed_two)
    grad_columns_low = grad_after_columns.astype(jnp.bfloat16)
    grad_proj, unused = section_backward(normed_cols_low, grad_columns_low, column_project, column_output, None, item_loop, head_loop)
    raw_column_output = product('bhld,blc->hdc', column_gated, grad_columns_low).reshape(H * DH, C)
    raw_column_project = product('blc,bfhld->cfhd', normed_cols_low, grad_proj).reshape(C, 4, H * DH)
    grad_normed_cols = product('bfhld,cfhd->blc', grad_proj, column_project.reshape(C, 4, H, DH))
    grad_after_rows = (grad_after_columns + norm_back(normed_cols, scale_cols, grad_normed_cols)).astype(jnp.bfloat16)
    return (grad_after_rows, raw_column_project, raw_column_output, raw_trans_in, raw_trans_out)

def row_block(normed_rows, scale_rows, normed_rows_low, row_gated, grad_after_rows, row_project, row_output, bias_table, head_loop):
    grad_proj, bias_total = section_backward(normed_rows_low, grad_after_rows, row_project, row_output, bias_table, True, head_loop)
    raw_row_output = product('bhld,blc->hdc', row_gated, grad_after_rows).reshape(H * DH, C)
    raw_row_project = product('blc,bfhld->cfhd', normed_rows_low, grad_proj).reshape(C, 4, H * DH)
    grad_normed_rows = product('bfhld,cfhd->blc', grad_proj, row_project.reshape(C, 4, H, DH))
    grad_alignment = (grad_after_rows.astype(jnp.float32) + norm_back(normed_rows, scale_rows, grad_normed_rows)).astype(jnp.bfloat16)
    return (grad_alignment, raw_row_project, raw_row_output, bias_total)

def reference(alignment, pair_bias, row_project, row_output, column_project, column_output, transition_in, transition_out, cotangent):
    normed_rows, scale_rows = normalize(alignment)
    normed_rows_low = normed_rows.astype(jnp.bfloat16)
    row_gated = section_forward(normed_rows_low, row_project, pair_bias, True, False)
    row_update = product('bhld,hdc->blc', row_gated, row_output.reshape(H, DH, C))
    after_rows = (alignment.astype(jnp.float32) + row_update).astype(jnp.bfloat16)
    columns = jnp.swapaxes(after_rows, 0, 1)
    upstream = jnp.swapaxes(cotangent, 0, 1)
    grad_columns, raw_column_project, raw_column_output, raw_trans_in, raw_trans_out = column_block(columns, upstream, column_project, column_output, transition_in, transition_out, True, False)
    grad_after_rows = jnp.swapaxes(grad_columns, 0, 1)
    grad_alignment, raw_row_project, raw_row_output, bias_total = row_block(normed_rows, scale_rows, normed_rows_low, row_gated, grad_after_rows, row_project, row_output, pair_bias, False)
    token_scale = (S * R) ** (-0.5)
    grad_bias = bias_total * (R * S ** (-0.5))
    return (grad_alignment, grad_bias, raw_row_project * token_scale, raw_row_output * token_scale, raw_column_project * token_scale, raw_column_output * token_scale, raw_trans_in * token_scale, raw_trans_out * token_scale)
```

```python
import jax
import jax.numpy as jnp
from jax import lax
from jax.experimental import pallas as pl
from jax.experimental.pallas import tpu as pltpu
from jax.sharding import PartitionSpec as P

C = 256
H = 8
DH = 32


EPSILON = 1e-05


def product(pattern, former, latter):
    return jnp.einsum(pattern, former, latter, preferred_element_type=jnp.float32)


def normalize(values):
    values = values.astype(jnp.float32)
    centred = values - jnp.mean(values, axis=-1, keepdims=True)
    factor = lax.rsqrt(jnp.mean(centred * centred, axis=-1, keepdims=True) + EPSILON)
    return (centred * factor, factor)


def norm_back(normed, factor, upstream):
    mean_up = jnp.mean(upstream, axis=-1, keepdims=True)
    mean_cross = jnp.mean(upstream * normed, axis=-1, keepdims=True)
    return factor * (upstream - mean_up - normed * mean_cross)


def run_items(function, arrays, sequential):
    if sequential:
        return lax.map(lambda bundle: function(*bundle), arrays)
    return jax.vmap(function)(*arrays)


def head_shares(queries, key_rows, bias_head):
    scores = product("qd,kd->qk", queries, key_rows)
    if bias_head is not None:
        scores = scores + bias_head.astype(jnp.float32)
    row_top = jnp.max(scores, axis=-1, keepdims=True)
    powered = jnp.exp(scores - row_top)
    return powered / jnp.sum(powered, axis=-1, keepdims=True)


def head_forward(queries, key_rows, values, bias_head=None):
    shares = head_shares(queries, key_rows, bias_head)
    return product("qk,kd->qd", shares.astype(jnp.bfloat16), values)


def head_backward(queries, key_rows, values, grad_blend, bias_head=None):
    shares = head_shares(queries, key_rows, bias_head)
    shares_low = shares.astype(jnp.bfloat16)
    blended = product("qk,kd->qd", shares_low, values)
    grad_shares = product("qd,kd->qk", grad_blend, values)
    grad_values = product("qk,qd->kd", shares_low, grad_blend)
    centre = jnp.sum(shares * grad_shares, axis=-1, keepdims=True)
    grad_scores = shares * (grad_shares - centre)
    grad_low = grad_scores.astype(jnp.bfloat16)
    grad_queries = product("qk,kd->qd", grad_low, key_rows)
    grad_keys = product("qk,qd->kd", grad_low, queries)
    return (blended, grad_queries, grad_keys, grad_values, grad_scores)


def item_project(normed_item, weights):
    projected = product("lc,cfhd->fhld", normed_item, weights.reshape(C, 4, H, DH))
    queries = (projected[0] * DH ** (-0.5)).astype(jnp.bfloat16)
    key_rows = projected[1].astype(jnp.bfloat16)
    values = projected[2].astype(jnp.bfloat16)
    gating = jax.nn.sigmoid(projected[3])
    return (queries, key_rows, values, gating)


def forward_item(normed_item, weights, bias_table, head_loop):
    queries, key_rows, values, gating = item_project(normed_item, weights)
    if bias_table is None:
        head_args = (queries, key_rows, values)
    else:
        head_args = (queries, key_rows, values, bias_table)
    blended = run_items(head_forward, head_args, head_loop)
    return (blended * gating).astype(jnp.bfloat16)


def backward_item(normed_item, upstream_item, weights, out_weight, bias_table, head_loop):
    queries, key_rows, values, gating = item_project(normed_item, weights)
    grad_gated = product("lc,hdc->hld", upstream_item, out_weight.reshape(H, DH, C))
    grad_blend = (grad_gated * gating).astype(jnp.bfloat16)
    if bias_table is None:
        head_args = (queries, key_rows, values, grad_blend)
    else:
        head_args = (queries, key_rows, values, grad_blend, bias_table)
    blended, grad_queries, grad_keys, grad_values, grad_scores = run_items(
        head_backward, head_args, head_loop
    )
    grad_gate = grad_gated * blended * gating * (1.0 - gating)
    grad_proj = jnp.stack(
        [grad_queries * DH ** (-0.5), grad_keys, grad_values, grad_gate], axis=0
    ).astype(jnp.bfloat16)
    if bias_table is None:
        return (grad_proj, jnp.zeros((), jnp.float32))
    return (grad_proj, grad_scores)


def section_forward(normed_low, weights, bias_table, item_loop, head_loop):

    def single(normed_item):
        return forward_item(normed_item, weights, bias_table, head_loop)

    return run_items(single, (normed_low,), item_loop)


def section_backward(
    normed_low, upstream_low, weights, out_weight, bias_table, item_loop, head_loop
):

    def single(normed_item, upstream_item):
        return backward_item(normed_item, upstream_item, weights, out_weight, bias_table, head_loop)

    if bias_table is None:
        grad_proj, unused = run_items(single, (normed_low, upstream_low), item_loop)
        return (grad_proj, None)

    def accumulate(running, bundle):
        grad_proj, grad_scores = single(bundle[0], bundle[1])
        return (running + grad_scores, grad_proj)

    bias_total, grad_proj = lax.scan(
        accumulate, jnp.zeros(bias_table.shape, jnp.float32), (normed_low, upstream_low)
    )
    return (grad_proj, bias_total)


def column_block(columns, upstream, column_project, column_output, transition_in, transition_out):
    normed_cols, scale_cols = normalize(columns)
    normed_cols_low = normed_cols.astype(jnp.bfloat16)
    column_gated = section_forward(normed_cols_low, column_project, None, False, False)
    column_update = product("bhld,hdc->blc", column_gated, column_output.reshape(H, DH, C))
    after_columns = (columns.astype(jnp.float32) + column_update).astype(jnp.bfloat16)
    normed_two, scale_two = normalize(after_columns)
    normed_two_low = normed_two.astype(jnp.bfloat16)
    pre_hidden = product("blc,cfe->blfe", normed_two_low, transition_in)
    gate_part = pre_hidden[:, :, 0]
    up_part = pre_hidden[:, :, 1]
    sigmoid_gate = jax.nn.sigmoid(gate_part)
    activated = gate_part * sigmoid_gate
    hidden = (activated * up_part).astype(jnp.bfloat16)
    raw_trans_out = product("blf,blc->fc", hidden, upstream)
    grad_hidden = product("blc,fc->blf", upstream, transition_out)
    grad_gate_part = grad_hidden * up_part * sigmoid_gate * (1.0 + gate_part * (1.0 - sigmoid_gate))
    grad_up_part = grad_hidden * activated
    grad_pre = jnp.stack([grad_gate_part, grad_up_part], axis=2).astype(jnp.bfloat16)
    raw_trans_in = product("blc,blfe->cfe", normed_two_low, grad_pre)
    grad_normed_two = product("blfe,cfe->blc", grad_pre, transition_in)
    grad_after_columns = upstream.astype(jnp.float32) + norm_back(
        normed_two, scale_two, grad_normed_two
    )
    grad_columns_low = grad_after_columns.astype(jnp.bfloat16)
    grad_proj, unused = section_backward(
        normed_cols_low, grad_columns_low, column_project, column_output, None, False, False
    )
    raw_column_output = product("bhld,blc->hdc", column_gated, grad_columns_low).reshape(H * DH, C)
    raw_column_project = product("blc,bfhld->cfhd", normed_cols_low, grad_proj).reshape(
        C, 4, H * DH
    )
    grad_normed_cols = product("bfhld,cfhd->blc", grad_proj, column_project.reshape(C, 4, H, DH))
    grad_after_rows = (
        grad_after_columns + norm_back(normed_cols, scale_cols, grad_normed_cols)
    ).astype(jnp.bfloat16)
    return (grad_after_rows, raw_column_project, raw_column_output, raw_trans_in, raw_trans_out)


def row_block(
    normed_rows,
    scale_rows,
    normed_rows_low,
    row_gated,
    grad_after_rows,
    row_project,
    row_output,
    bias_table,
):
    grad_proj, bias_total = section_backward(
        normed_rows_low, grad_after_rows, row_project, row_output, bias_table, True, True
    )
    raw_row_output = product("bhld,blc->hdc", row_gated, grad_after_rows).reshape(H * DH, C)
    raw_row_project = product("blc,bfhld->cfhd", normed_rows_low, grad_proj).reshape(C, 4, H * DH)
    grad_normed_rows = product("bfhld,cfhd->blc", grad_proj, row_project.reshape(C, 4, H, DH))
    grad_alignment = (
        grad_after_rows.astype(jnp.float32) + norm_back(normed_rows, scale_rows, grad_normed_rows)
    ).astype(jnp.bfloat16)
    return (grad_alignment, raw_row_project, raw_row_output, bias_total)


def to_columns(arranged):
    moved = lax.all_to_all(arranged, ("dap", "sub"), split_axis=1, concat_axis=0, tiled=True)
    return moved


def to_rows(arranged):
    moved = lax.all_to_all(arranged, ("dap", "sub"), split_axis=0, concat_axis=1, tiled=True)
    return moved


def distributed(
    alignment,
    pair_bias,
    row_project,
    row_output,
    column_project,
    column_output,
    transition_in,
    transition_out,
    cotangent,
):
    bias_full = lax.all_gather(pair_bias, ("dap", "sub"), axis=1, tiled=True)
    upstream = jnp.swapaxes(to_columns(cotangent), 0, 1)
    normed_rows, scale_rows = normalize(alignment)
    normed_rows_low = normed_rows.astype(jnp.bfloat16)
    row_gated = section_forward(normed_rows_low, row_project, bias_full, True, True)
    row_update = product("bhld,hdc->blc", row_gated, row_output.reshape(H, DH, C))
    after_rows = (alignment.astype(jnp.float32) + row_update).astype(jnp.bfloat16)
    columns = jnp.swapaxes(to_columns(after_rows), 0, 1)
    grad_columns, raw_column_project, raw_column_output, raw_trans_in, raw_trans_out = column_block(
        columns, upstream, column_project, column_output, transition_in, transition_out
    )
    sequences = alignment.shape[0] * lax.axis_size("dap") * lax.axis_size("sub")
    residues = alignment.shape[1]
    token_scale = (sequences * residues) ** (-0.5)
    term_col_project = raw_column_project * token_scale
    term_col_output = raw_column_output * token_scale
    term_trans_in = raw_trans_in * token_scale
    term_trans_out = raw_trans_out * token_scale
    grad_after_rows = to_rows(jnp.swapaxes(grad_columns, 0, 1))
    grad_alignment, raw_row_project, raw_row_output, bias_total = row_block(
        normed_rows,
        scale_rows,
        normed_rows_low,
        row_gated,
        grad_after_rows,
        row_project,
        row_output,
        bias_full,
    )
    term_row_project = raw_row_project * token_scale
    term_row_output = raw_row_output * token_scale
    bias_term = bias_total * (residues * sequences ** (-0.5))
    grad_bias = lax.psum_scatter(bias_term, ("dap", "sub"), scatter_dimension=1, tiled=True)
    (
        grad_row_project,
        grad_row_output,
        grad_col_project,
        grad_col_output,
        grad_trans_in,
        grad_trans_out,
    ) = (
        lax.psum_scatter(term_row_project, ("dap", "sub"), scatter_dimension=0, tiled=True),
        lax.psum_scatter(term_row_output, ("dap", "sub"), scatter_dimension=0, tiled=True),
        lax.psum_scatter(term_col_project, ("dap", "sub"), scatter_dimension=0, tiled=True),
        lax.psum_scatter(term_col_output, ("dap", "sub"), scatter_dimension=0, tiled=True),
        lax.psum_scatter(term_trans_in, ("dap", "sub"), scatter_dimension=0, tiled=True),
        lax.psum_scatter(term_trans_out, ("dap", "sub"), scatter_dimension=0, tiled=True),
    )
    return (
        grad_alignment,
        grad_bias,
        grad_row_project,
        grad_row_output,
        grad_col_project,
        grad_col_output,
        grad_trans_in,
        grad_trans_out,
    )


GATHERED_HIDDEN_BYTES = 8 * 2**20


def dot_nn(former, latter):
    return lax.dot_general(
        former, latter, (((1,), (0,)), ((), ())), preferred_element_type=jnp.float32
    )


def dot_nt(former, latter):
    return lax.dot_general(
        former, latter, (((1,), (1,)), ((), ())), preferred_element_type=jnp.float32
    )


def dot_tn(former, latter):
    return lax.dot_general(
        former, latter, (((0,), (0,)), ((), ())), preferred_element_type=jnp.float32
    )


def iota(shape, axis):
    return lax.broadcasted_iota(jnp.int32, shape, axis)


def one_hot(condition):
    return jnp.where(condition, 1.0, 0.0).astype(jnp.bfloat16)


def segments(values, length, join):
    width = values.shape[-1]
    place = iota(values.shape, 1) % length
    step = 1
    while step < length:
        ahead = pltpu.roll(values, width - step, 1)
        around = pltpu.roll(values, length - step, 1)
        values = join(values, jnp.where(place < length - step, ahead, around))
        step *= 2
    return values


def by_head(rows, length):
    tall = jnp.concatenate([rows] * H, axis=0)
    own = iota(tall.shape, 0) // length == iota(tall.shape, 1) // DH
    return jnp.where(own, tall, jnp.zeros_like(tall))


def from_heads(tall, length):
    head = iota((length, tall.shape[1]), 1) // DH
    kept = tall[:length]
    for at in range(1, H):
        kept = jnp.where(head == at, tall[at * length : (at + 1) * length], kept)
    return kept


def part_rows(values, length):
    return [values[at : at + length] for at in range(0, values.shape[0], length)]


def attend(normed_low, weights, bias_rows, length):
    projected = [dot_nn(normed_low, weights[:, at * C : (at + 1) * C]) for at in range(4)]
    queries = (projected[0] * DH ** (-0.5)).astype(jnp.bfloat16)
    key_rows = projected[1].astype(jnp.bfloat16)
    values = projected[2].astype(jnp.bfloat16)
    gating = jax.nn.sigmoid(projected[3])
    scores = jnp.concatenate(
        [
            dot_nt(query, by_head(key, length))
            for query, key in zip(part_rows(queries, length), part_rows(key_rows, length))
        ],
        axis=0,
    )
    if bias_rows is not None:
        scores = scores + jnp.concatenate([bias_rows] * (scores.shape[0] // length), axis=0)
    powered = jnp.exp(scores - segments(scores, length, jnp.maximum))
    shares = powered / segments(powered, length, jnp.add)
    shares_low = shares.astype(jnp.bfloat16)
    blended = jnp.concatenate(
        [
            dot_nn(share, by_head(value, length))
            for share, value in zip(part_rows(shares_low, length), part_rows(values, length))
        ],
        axis=0,
    )
    gated = (blended * gating).astype(jnp.bfloat16)
    return gated, (queries, key_rows, values, gating, shares, shares_low, blended)


def attend_back(saved, upstream_low, out_weight, length):
    queries, key_rows, values, gating, shares, shares_low, blended = saved
    grad_gated = dot_nt(upstream_low, out_weight)
    grad_blend = (grad_gated * gating).astype(jnp.bfloat16)
    grad_shares = jnp.concatenate(
        [
            dot_nt(grad, by_head(value, length))
            for grad, value in zip(part_rows(grad_blend, length), part_rows(values, length))
        ],
        axis=0,
    )
    grad_scores = shares * (grad_shares - segments(shares * grad_shares, length, jnp.add))
    grad_low = grad_scores.astype(jnp.bfloat16)
    grad_queries = []
    grad_keys = []
    grad_values = []
    for score, key, query, share, grad in zip(
        part_rows(grad_low, length),
        part_rows(key_rows, length),
        part_rows(queries, length),
        part_rows(shares_low, length),
        part_rows(grad_blend, length),
    ):
        grad_queries.append(dot_nn(score, by_head(key, length)))
        grad_keys.append(from_heads(dot_tn(score, query), length))
        grad_values.append(from_heads(dot_tn(share, grad), length))
    grad_gate = grad_gated * blended * gating * (1.0 - gating)
    grad_proj = jnp.concatenate(
        [
            (jnp.concatenate(grad_queries, axis=0) * DH ** (-0.5)).astype(jnp.bfloat16),
            jnp.concatenate(grad_keys, axis=0).astype(jnp.bfloat16),
            jnp.concatenate(grad_values, axis=0).astype(jnp.bfloat16),
            grad_gate.astype(jnp.bfloat16),
        ],
        axis=1,
    )
    return grad_proj, grad_scores


def sample_kernel(
    place_ref,
    gathered_ref,
    row_project_ref,
    row_output_ref,
    column_project_ref,
    column_output_ref,
    transition_in_ref,
    transition_out_ref,
    grad_alignment_ref,
    grad_bias_ref,
    grad_row_project_ref,
    grad_row_output_ref,
    grad_column_project_ref,
    grad_column_output_ref,
    grad_transition_in_ref,
    grad_transition_out_ref,
    *,
    daps,
    subs,
    residues,
):
    sequences = gathered_ref.shape[0]
    tokens = sequences * residues
    hidden_units = transition_out_ref.shape[0]
    token_scale = tokens ** (-0.5)
    dap = place_ref[0]
    sub = place_ref[1]
    own = dap * subs + sub

    def chosen(values, count):
        shape = (count, values.shape[1])
        picked = one_hot(iota(shape, 1) == iota(shape, 0) + own * count)
        return dot_nt(picked, values).astype(jnp.bfloat16)

    alignment = gathered_ref[:, :residues, :].reshape(tokens, C)
    cotangent = gathered_ref[:, residues : 2 * residues, :].reshape(tokens, C)
    lanes = H * residues
    bias_blocks = gathered_ref[:, 2 * residues, :lanes]
    from_place = iota((residues, sequences), 1)
    from_dap = dap - from_place // subs
    from_dap = jnp.where(from_dap < 0, from_dap + daps, from_dap)
    from_sub = sub - from_place % subs
    from_sub = jnp.where(from_sub < 0, from_sub + subs, from_sub)
    bias_order = one_hot(from_dap * subs + from_sub == iota((residues, sequences), 0))
    bias_rows = dot_nn(bias_order, bias_blocks)
    turn = iota((tokens, tokens), 0)
    to_columns = one_hot(
        iota((tokens, tokens), 1) == (turn % sequences) * residues + turn // sequences
    )

    row_weights = row_project_ref[...]
    values_in = alignment.astype(jnp.float32)
    normed_rows, scale_rows = normalize(values_in)
    normed_rows_low = normed_rows.astype(jnp.bfloat16)
    row_gated, row_saved = attend(normed_rows_low, row_weights, bias_rows, residues)
    after_rows = (values_in + dot_nn(row_gated, row_output_ref[...])).astype(jnp.bfloat16)

    column_weights = column_project_ref[...]
    columns = dot_nn(to_columns, after_rows)
    upstream = dot_nn(to_columns, cotangent)
    upstream_low = upstream.astype(jnp.bfloat16)
    normed_cols, scale_cols = normalize(columns)
    normed_cols_low = normed_cols.astype(jnp.bfloat16)
    column_gated, column_saved = attend(normed_cols_low, column_weights, None, sequences)
    after_columns = (columns + dot_nn(column_gated, column_output_ref[...])).astype(jnp.bfloat16)

    normed_two, scale_two = normalize(after_columns)
    normed_two_low = normed_two.astype(jnp.bfloat16)
    chosen_two = chosen(normed_two_low, C // sequences)
    unit_rows = hidden_units // sequences
    chunk = min(C, hidden_units)
    chosen_hidden = None
    grad_normed_two = None
    for at in range(0, hidden_units, chunk):
        gate_weight = transition_in_ref[:, at : at + chunk]
        up_weight = transition_in_ref[:, hidden_units + at : hidden_units + at + chunk]
        gate_part = dot_nn(normed_two_low, gate_weight)
        up_part = dot_nn(normed_two_low, up_weight)
        grad_hidden = dot_nt(upstream_low, transition_out_ref[at : at + chunk, :])
        sigmoid_gate = jax.nn.sigmoid(gate_part)
        activated = gate_part * sigmoid_gate
        hidden = (activated * up_part).astype(jnp.bfloat16)
        grad_gate_part = (
            grad_hidden * up_part * sigmoid_gate * (1.0 + gate_part * (1.0 - sigmoid_gate))
        ).astype(jnp.bfloat16)
        grad_up_part = (grad_hidden * activated).astype(jnp.bfloat16)
        shape = (unit_rows, chunk)
        picked = one_hot(iota(shape, 1) + at == iota(shape, 0) + own * unit_rows)
        part = dot_nt(picked, hidden)
        chosen_hidden = part if chosen_hidden is None else chosen_hidden + part
        part = dot_nt(grad_gate_part, gate_weight) + dot_nt(grad_up_part, up_weight)
        grad_normed_two = part if grad_normed_two is None else grad_normed_two + part
        grad_transition_in_ref[:, 0, at : at + chunk] = (
            dot_nn(chosen_two, grad_gate_part) * token_scale
        )
        grad_transition_in_ref[:, 1, at : at + chunk] = (
            dot_nn(chosen_two, grad_up_part) * token_scale
        )
    grad_transition_out_ref[...] = (
        dot_nn(chosen_hidden.astype(jnp.bfloat16), upstream_low) * token_scale
    )
    grad_after_columns = upstream + norm_back(normed_two, scale_two, grad_normed_two)

    grad_columns_low = grad_after_columns.astype(jnp.bfloat16)
    column_grad_proj, unused = attend_back(
        column_saved, grad_columns_low, column_output_ref[...], sequences
    )
    grad_column_output_ref[...] = (
        dot_nn(chosen(column_gated, C // sequences), grad_columns_low) * token_scale
    )
    raw = dot_nn(chosen(normed_cols_low, C // sequences), column_grad_proj) * token_scale
    for at in range(4):
        grad_column_project_ref[:, at, :] = raw[:, at * C : (at + 1) * C]
    grad_normed_cols = dot_nt(column_grad_proj, column_weights)
    grad_turned = (
        grad_after_columns + norm_back(normed_cols, scale_cols, grad_normed_cols)
    ).astype(jnp.bfloat16)

    grad_after_rows = dot_tn(to_columns, grad_turned)
    grad_rows_low = grad_after_rows.astype(jnp.bfloat16)
    row_grad_proj, row_grad_scores = attend_back(
        row_saved, grad_rows_low, row_output_ref[...], residues
    )
    grad_row_output_ref[...] = (
        dot_nn(chosen(row_gated, C // sequences), grad_rows_low) * token_scale
    )
    raw = dot_nn(chosen(normed_rows_low, C // sequences), row_grad_proj) * token_scale
    for at in range(4):
        grad_row_project_ref[:, at, :] = raw[:, at * C : (at + 1) * C]
    bias_total = sum(part_rows(row_grad_scores, residues)) * (residues * sequences ** (-0.5))
    bias_own = jnp.sum(
        jnp.where(iota(bias_total.shape, 0) == own, bias_total, 0.0), axis=0, keepdims=True
    )
    for at in range(H):
        grad_bias_ref[at : at + 1, 0, :] = bias_own[:, at * residues : (at + 1) * residues]
    grad_normed_rows = dot_nt(row_grad_proj[:residues], row_weights)
    grad_alignment_ref[0] = (
        grad_after_rows[:residues]
        + norm_back(normed_rows[:residues], scale_rows[:residues], grad_normed_rows)
    ).astype(jnp.bfloat16)


def sample_call(daps, subs, residues, sequences, hidden_units):
    rows = C // sequences
    out_shape = (
        jax.ShapeDtypeStruct((1, residues, C), jnp.bfloat16),
        jax.ShapeDtypeStruct((H, 1, residues), jnp.float32),
        jax.ShapeDtypeStruct((rows, 4, H * DH), jnp.float32),
        jax.ShapeDtypeStruct((rows, C), jnp.float32),
        jax.ShapeDtypeStruct((rows, 4, H * DH), jnp.float32),
        jax.ShapeDtypeStruct((rows, C), jnp.float32),
        jax.ShapeDtypeStruct((rows, 2, hidden_units), jnp.float32),
        jax.ShapeDtypeStruct((hidden_units // sequences, C), jnp.float32),
    )
    return pl.pallas_call(
        lambda *refs: sample_kernel(*refs, daps=daps, subs=subs, residues=residues),
        out_shape=out_shape,
        in_specs=[pl.BlockSpec(memory_space=pltpu.SMEM)]
        + [pl.BlockSpec(memory_space=pltpu.VMEM)] * 7,
        out_specs=tuple(pl.BlockSpec(memory_space=pltpu.VMEM) for _ in out_shape),
        name="sample",
    )


def around(values, axis):
    size = lax.axis_size(axis)
    blocks = [values]
    for shift in range(1, size):
        pairs = [(source, (source + shift) % size) for source in range(size)]
        blocks.append(lax.ppermute(values, axis, pairs))
    return jnp.concatenate(blocks, axis=0)


def gathered(
    alignment,
    pair_bias,
    row_project,
    row_output,
    column_project,
    column_output,
    transition_in,
    transition_out,
    cotangent,
):
    daps = lax.axis_size("dap")
    subs = lax.axis_size("sub")
    residues = alignment.shape[1]
    hidden_units = transition_out.shape[0]
    bias_row = jnp.pad(pair_bias.reshape(1, 1, H * residues), ((0, 0), (0, 0), (0, C - H * residues)))
    block = jnp.concatenate([alignment, cotangent, bias_row], axis=1)
    blocks = around(around(block, "sub"), "dap")
    place = jnp.stack([lax.axis_index("dap"), lax.axis_index("sub")]).astype(jnp.int32)
    return sample_call(daps, subs, residues, daps * subs, hidden_units)(
        place,
        blocks,
        row_project.reshape(C, 4 * H * DH),
        row_output,
        column_project.reshape(C, 4 * H * DH),
        column_output,
        transition_in.reshape(C, 2 * hidden_units),
        transition_out,
    )


def gathered_fits(alignment, transition_out):
    sequences = alignment.shape[0] * lax.axis_size("dap") * lax.axis_size("sub")
    residues = alignment.shape[1]
    hidden_bytes = sequences * residues * 2 * transition_out.shape[0] * 4
    lengths_fit = all(
        length >= 16 and length & (length - 1) == 0 and H * length <= C
        for length in (sequences, residues)
    )
    return (
        alignment.shape[0] == 1
        and sequences == residues
        and lengths_fit
        and hidden_bytes <= GATHERED_HIDDEN_BYTES
    )


def shards(alignment, *others):
    transition_out = others[-2]
    plan = gathered if gathered_fits(alignment, transition_out) else distributed
    return plan(alignment, *others)


def solution(mesh):
    in_specs = (
        P(("grp", "dap", "sub"), None, None),
        P(None, ("grp", "dap", "sub"), None),
        P(),
        P(),
        P(),
        P(),
        P(),
        P(),
        P(("grp", "dap", "sub"), None, None),
    )
    out_specs = (
        P(("grp", "dap", "sub"), None, None),
        P(None, ("grp", "dap", "sub"), None),
        P(("grp", "dap", "sub"), None, None),
        P(("grp", "dap", "sub"), None),
        P(("grp", "dap", "sub"), None, None),
        P(("grp", "dap", "sub"), None),
        P(("grp", "dap", "sub"), None, None),
        P(("grp", "dap", "sub"), None),
    )
    return jax.shard_map(shards, mesh=mesh, in_specs=in_specs, out_specs=out_specs, check_vma=False)
```

```python
import jax
import jax.numpy as jnp
from jax import lax
from jax.experimental import pallas as pl
from jax.experimental.pallas import tpu as pltpu
from jax.sharding import PartitionSpec as P

C = 256
H = 8
DH = 32


EPSILON = 1e-05


def product(pattern, former, latter):
    return jnp.einsum(pattern, former, latter, preferred_element_type=jnp.float32)


def normalize(values):
    values = values.astype(jnp.float32)
    centred = values - jnp.mean(values, axis=-1, keepdims=True)
    factor = lax.rsqrt(jnp.mean(centred * centred, axis=-1, keepdims=True) + EPSILON)
    return (centred * factor, factor)


def norm_back(normed, factor, upstream):
    mean_up = jnp.mean(upstream, axis=-1, keepdims=True)
    mean_cross = jnp.mean(upstream * normed, axis=-1, keepdims=True)
    return factor * (upstream - mean_up - normed * mean_cross)


def run_items(function, arrays, sequential):
    if sequential:
        return lax.map(lambda bundle: function(*bundle), arrays)
    return jax.vmap(function)(*arrays)


def head_shares(queries, key_rows, bias_head):
    scores = product("qd,kd->qk", queries, key_rows)
    if bias_head is not None:
        scores = scores + bias_head.astype(jnp.float32)
    row_top = jnp.max(scores, axis=-1, keepdims=True)
    powered = jnp.exp(scores - row_top)
    return powered / jnp.sum(powered, axis=-1, keepdims=True)


def head_forward(queries, key_rows, values, bias_head=None):
    shares = head_shares(queries, key_rows, bias_head)
    return product("qk,kd->qd", shares.astype(jnp.bfloat16), values)


def head_backward(queries, key_rows, values, grad_blend, bias_head=None):
    shares = head_shares(queries, key_rows, bias_head)
    shares_low = shares.astype(jnp.bfloat16)
    blended = product("qk,kd->qd", shares_low, values)
    grad_shares = product("qd,kd->qk", grad_blend, values)
    grad_values = product("qk,qd->kd", shares_low, grad_blend)
    centre = jnp.sum(shares * grad_shares, axis=-1, keepdims=True)
    grad_scores = shares * (grad_shares - centre)
    grad_low = grad_scores.astype(jnp.bfloat16)
    grad_queries = product("qk,kd->qd", grad_low, key_rows)
    grad_keys = product("qk,qd->kd", grad_low, queries)
    return (blended, grad_queries, grad_keys, grad_values, grad_scores)


def item_project(normed_item, weights):
    projected = product("lc,cfhd->fhld", normed_item, weights.reshape(C, 4, H, DH))
    queries = (projected[0] * DH ** (-0.5)).astype(jnp.bfloat16)
    key_rows = projected[1].astype(jnp.bfloat16)
    values = projected[2].astype(jnp.bfloat16)
    gating = jax.nn.sigmoid(projected[3])
    return (queries, key_rows, values, gating)


def forward_item(normed_item, weights, bias_table, head_loop):
    queries, key_rows, values, gating = item_project(normed_item, weights)
    if bias_table is None:
        head_args = (queries, key_rows, values)
    else:
        head_args = (queries, key_rows, values, bias_table)
    blended = run_items(head_forward, head_args, head_loop)
    return (blended * gating).astype(jnp.bfloat16)


def backward_item(normed_item, upstream_item, weights, out_weight, bias_table, head_loop):
    queries, key_rows, values, gating = item_project(normed_item, weights)
    grad_gated = product("lc,hdc->hld", upstream_item, out_weight.reshape(H, DH, C))
    grad_blend = (grad_gated * gating).astype(jnp.bfloat16)
    if bias_table is None:
        head_args = (queries, key_rows, values, grad_blend)
    else:
        head_args = (queries, key_rows, values, grad_blend, bias_table)
    blended, grad_queries, grad_keys, grad_values, grad_scores = run_items(
        head_backward, head_args, head_loop
    )
    grad_gate = grad_gated * blended * gating * (1.0 - gating)
    grad_proj = jnp.stack(
        [grad_queries * DH ** (-0.5), grad_keys, grad_values, grad_gate], axis=0
    ).astype(jnp.bfloat16)
    if bias_table is None:
        return (grad_proj, jnp.zeros((), jnp.float32))
    return (grad_proj, grad_scores)


def section_forward(normed_low, weights, bias_table, item_loop, head_loop):

    def single(normed_item):
        return forward_item(normed_item, weights, bias_table, head_loop)

    return run_items(single, (normed_low,), item_loop)


def section_backward(
    normed_low, upstream_low, weights, out_weight, bias_table, item_loop, head_loop
):

    def single(normed_item, upstream_item):
        return backward_item(normed_item, upstream_item, weights, out_weight, bias_table, head_loop)

    if bias_table is None:
        grad_proj, unused = run_items(single, (normed_low, upstream_low), item_loop)
        return (grad_proj, None)

    def accumulate(running, bundle):
        grad_proj, grad_scores = single(bundle[0], bundle[1])
        return (running + grad_scores, grad_proj)

    bias_total, grad_proj = lax.scan(
        accumulate, jnp.zeros(bias_table.shape, jnp.float32), (normed_low, upstream_low)
    )
    return (grad_proj, bias_total)


def column_block(columns, upstream, column_project, column_output, transition_in, transition_out):
    normed_cols, scale_cols = normalize(columns)
    normed_cols_low = normed_cols.astype(jnp.bfloat16)
    column_gated = section_forward(normed_cols_low, column_project, None, False, False)
    column_update = product("bhld,hdc->blc", column_gated, column_output.reshape(H, DH, C))
    after_columns = (columns.astype(jnp.float32) + column_update).astype(jnp.bfloat16)
    normed_two, scale_two = normalize(after_columns)
    normed_two_low = normed_two.astype(jnp.bfloat16)
    pre_hidden = product("blc,cfe->blfe", normed_two_low, transition_in)
    gate_part = pre_hidden[:, :, 0]
    up_part = pre_hidden[:, :, 1]
    sigmoid_gate = jax.nn.sigmoid(gate_part)
    activated = gate_part * sigmoid_gate
    hidden = (activated * up_part).astype(jnp.bfloat16)
    raw_trans_out = product("blf,blc->fc", hidden, upstream)
    grad_hidden = product("blc,fc->blf", upstream, transition_out)
    grad_gate_part = grad_hidden * up_part * sigmoid_gate * (1.0 + gate_part * (1.0 - sigmoid_gate))
    grad_up_part = grad_hidden * activated
    grad_pre = jnp.stack([grad_gate_part, grad_up_part], axis=2).astype(jnp.bfloat16)
    raw_trans_in = product("blc,blfe->cfe", normed_two_low, grad_pre)
    grad_normed_two = product("blfe,cfe->blc", grad_pre, transition_in)
    grad_after_columns = upstream.astype(jnp.float32) + norm_back(
        normed_two, scale_two, grad_normed_two
    )
    grad_columns_low = grad_after_columns.astype(jnp.bfloat16)
    grad_proj, unused = section_backward(
        normed_cols_low, grad_columns_low, column_project, column_output, None, False, False
    )
    raw_column_output = product("bhld,blc->hdc", column_gated, grad_columns_low).reshape(H * DH, C)
    raw_column_project = product("blc,bfhld->cfhd", normed_cols_low, grad_proj).reshape(
        C, 4, H * DH
    )
    grad_normed_cols = product("bfhld,cfhd->blc", grad_proj, column_project.reshape(C, 4, H, DH))
    grad_after_rows = (
        grad_after_columns + norm_back(normed_cols, scale_cols, grad_normed_cols)
    ).astype(jnp.bfloat16)
    return (grad_after_rows, raw_column_project, raw_column_output, raw_trans_in, raw_trans_out)


def row_block(
    normed_rows,
    scale_rows,
    normed_rows_low,
    row_gated,
    grad_after_rows,
    row_project,
    row_output,
    bias_table,
):
    grad_proj, bias_total = section_backward(
        normed_rows_low, grad_after_rows, row_project, row_output, bias_table, True, True
    )
    raw_row_output = product("bhld,blc->hdc", row_gated, grad_after_rows).reshape(H * DH, C)
    raw_row_project = product("blc,bfhld->cfhd", normed_rows_low, grad_proj).reshape(C, 4, H * DH)
    grad_normed_rows = product("bfhld,cfhd->blc", grad_proj, row_project.reshape(C, 4, H, DH))
    grad_alignment = (
        grad_after_rows.astype(jnp.float32) + norm_back(normed_rows, scale_rows, grad_normed_rows)
    ).astype(jnp.bfloat16)
    return (grad_alignment, raw_row_project, raw_row_output, bias_total)


def to_columns(arranged):
    moved = lax.all_to_all(arranged, ("dap", "sub"), split_axis=1, concat_axis=0, tiled=True)
    return moved


def to_rows(arranged):
    moved = lax.all_to_all(arranged, ("dap", "sub"), split_axis=0, concat_axis=1, tiled=True)
    return moved


def distributed(
    alignment,
    pair_bias,
    row_project,
    row_output,
    column_project,
    column_output,
    transition_in,
    transition_out,
    cotangent,
):
    bias_full = lax.all_gather(pair_bias, ("dap", "sub"), axis=1, tiled=True)
    upstream = jnp.swapaxes(to_columns(cotangent), 0, 1)
    normed_rows, scale_rows = normalize(alignment)
    normed_rows_low = normed_rows.astype(jnp.bfloat16)
    row_gated = section_forward(normed_rows_low, row_project, bias_full, True, True)
    row_update = product("bhld,hdc->blc", row_gated, row_output.reshape(H, DH, C))
    after_rows = (alignment.astype(jnp.float32) + row_update).astype(jnp.bfloat16)
    columns = jnp.swapaxes(to_columns(after_rows), 0, 1)
    grad_columns, raw_column_project, raw_column_output, raw_trans_in, raw_trans_out = column_block(
        columns, upstream, column_project, column_output, transition_in, transition_out
    )
    sequences = alignment.shape[0] * lax.axis_size("dap") * lax.axis_size("sub")
    residues = alignment.shape[1]
    token_scale = (sequences * residues) ** (-0.5)
    term_col_project = raw_column_project * token_scale
    term_col_output = raw_column_output * token_scale
    term_trans_in = raw_trans_in * token_scale
    term_trans_out = raw_trans_out * token_scale
    grad_after_rows = to_rows(jnp.swapaxes(grad_columns, 0, 1))
    grad_alignment, raw_row_project, raw_row_output, bias_total = row_block(
        normed_rows,
        scale_rows,
        normed_rows_low,
        row_gated,
        grad_after_rows,
        row_project,
        row_output,
        bias_full,
    )
    term_row_project = raw_row_project * token_scale
    term_row_output = raw_row_output * token_scale
    bias_term = bias_total * (residues * sequences ** (-0.5))
    grad_bias = lax.psum_scatter(bias_term, ("dap", "sub"), scatter_dimension=1, tiled=True)
    (
        grad_row_project,
        grad_row_output,
        grad_col_project,
        grad_col_output,
        grad_trans_in,
        grad_trans_out,
    ) = (
        lax.psum_scatter(term_row_project, ("dap", "sub"), scatter_dimension=0, tiled=True),
        lax.psum_scatter(term_row_output, ("dap", "sub"), scatter_dimension=0, tiled=True),
        lax.psum_scatter(term_col_project, ("dap", "sub"), scatter_dimension=0, tiled=True),
        lax.psum_scatter(term_col_output, ("dap", "sub"), scatter_dimension=0, tiled=True),
        lax.psum_scatter(term_trans_in, ("dap", "sub"), scatter_dimension=0, tiled=True),
        lax.psum_scatter(term_trans_out, ("dap", "sub"), scatter_dimension=0, tiled=True),
    )
    return (
        grad_alignment,
        grad_bias,
        grad_row_project,
        grad_row_output,
        grad_col_project,
        grad_col_output,
        grad_trans_in,
        grad_trans_out,
    )


GATHERED_HIDDEN_BYTES = 8 * 2**20
KERNEL_VMEM_BYTES = 24 * 2**20


def dot_nn(former, latter):
    return lax.dot_general(
        former, latter, (((1,), (0,)), ((), ())), preferred_element_type=jnp.float32
    )


def dot_nt(former, latter):
    return lax.dot_general(
        former, latter, (((1,), (1,)), ((), ())), preferred_element_type=jnp.float32
    )


def dot_tn(former, latter):
    return lax.dot_general(
        former, latter, (((0,), (0,)), ((), ())), preferred_element_type=jnp.float32
    )


def iota(shape, axis):
    return lax.broadcasted_iota(jnp.int32, shape, axis)


def one_hot(condition):
    return jnp.where(condition, 1.0, 0.0).astype(jnp.bfloat16)


def segments(values, length, join):
    width = values.shape[-1]
    place = iota(values.shape, 1) % length
    step = 1
    while step < length:
        ahead = pltpu.roll(values, width - step, 1)
        around = pltpu.roll(values, length - step, 1)
        values = join(values, jnp.where(place < length - step, ahead, around))
        step *= 2
    return values


def by_head(rows, length):
    tall = jnp.concatenate([rows] * H, axis=0)
    own = iota(tall.shape, 0) // length == iota(tall.shape, 1) // DH
    return jnp.where(own, tall, jnp.zeros_like(tall))


def from_heads(tall, length):
    head = iota((length, tall.shape[1]), 1) // DH
    kept = tall[:length]
    for at in range(1, H):
        kept = jnp.where(head == at, tall[at * length : (at + 1) * length], kept)
    return kept


def part_rows(values, length):
    return [values[at : at + length] for at in range(0, values.shape[0], length)]


def attend(normed_low, weights, bias_rows, length):
    projected = [dot_nn(normed_low, weights[:, at * C : (at + 1) * C]) for at in range(4)]
    queries = (projected[0] * DH ** (-0.5)).astype(jnp.bfloat16)
    key_rows = projected[1].astype(jnp.bfloat16)
    values = projected[2].astype(jnp.bfloat16)
    gating = jax.nn.sigmoid(projected[3])
    scores = jnp.concatenate(
        [
            dot_nt(query, by_head(key, length))
            for query, key in zip(part_rows(queries, length), part_rows(key_rows, length))
        ],
        axis=0,
    )
    if bias_rows is not None:
        scores = scores + jnp.concatenate([bias_rows] * (scores.shape[0] // length), axis=0)
    powered = jnp.exp(scores - segments(scores, length, jnp.maximum))
    shares = powered / segments(powered, length, jnp.add)
    shares_low = shares.astype(jnp.bfloat16)
    blended = jnp.concatenate(
        [
            dot_nn(share, by_head(value, length))
            for share, value in zip(part_rows(shares_low, length), part_rows(values, length))
        ],
        axis=0,
    )
    gated = (blended * gating).astype(jnp.bfloat16)
    return gated, (queries, key_rows, values, gating, shares, shares_low, blended)


def attend_back(saved, upstream_low, out_weight, length):
    queries, key_rows, values, gating, shares, shares_low, blended = saved
    grad_gated = dot_nt(upstream_low, out_weight)
    grad_blend = (grad_gated * gating).astype(jnp.bfloat16)
    grad_shares = jnp.concatenate(
        [
            dot_nt(grad, by_head(value, length))
            for grad, value in zip(part_rows(grad_blend, length), part_rows(values, length))
        ],
        axis=0,
    )
    grad_scores = shares * (grad_shares - segments(shares * grad_shares, length, jnp.add))
    grad_low = grad_scores.astype(jnp.bfloat16)
    grad_queries = []
    grad_keys = []
    grad_values = []
    for score, key, query, share, grad in zip(
        part_rows(grad_low, length),
        part_rows(key_rows, length),
        part_rows(queries, length),
        part_rows(shares_low, length),
        part_rows(grad_blend, length),
    ):
        grad_queries.append(dot_nn(score, by_head(key, length)))
        grad_keys.append(from_heads(dot_tn(score, query), length))
        grad_values.append(from_heads(dot_tn(share, grad), length))
    grad_gate = grad_gated * blended * gating * (1.0 - gating)
    grad_proj = jnp.concatenate(
        [
            (jnp.concatenate(grad_queries, axis=0) * DH ** (-0.5)).astype(jnp.bfloat16),
            jnp.concatenate(grad_keys, axis=0).astype(jnp.bfloat16),
            jnp.concatenate(grad_values, axis=0).astype(jnp.bfloat16),
            grad_gate.astype(jnp.bfloat16),
        ],
        axis=1,
    )
    return grad_proj, grad_scores


def sample_kernel(
    gathered_ref,
    row_project_ref,
    column_project_ref,
    transition_in_ref,
    outputs_ref,
    grad_alignment_ref,
    grad_bias_ref,
    grad_row_project_ref,
    grad_row_output_ref,
    grad_column_project_ref,
    grad_column_output_ref,
    grad_transition_in_ref,
    grad_transition_out_ref,
    *,
    daps,
    subs,
    residues,
):
    sequences = gathered_ref.shape[0]
    tokens = sequences * residues
    hidden_units = transition_in_ref.shape[1] // 2
    token_scale = tokens ** (-0.5)
    dap = lax.axis_index("dap")
    sub = lax.axis_index("sub")
    own = dap * subs + sub

    def chosen(values, count):
        shape = (count, values.shape[1])
        picked = one_hot(iota(shape, 1) == iota(shape, 0) + own * count)
        return dot_nt(picked, values).astype(jnp.bfloat16)

    alignment = gathered_ref[:, :residues, :].reshape(tokens, C)
    cotangent = gathered_ref[:, residues : 2 * residues, :].reshape(tokens, C)
    lanes = H * residues
    bias_blocks = gathered_ref[:, 2 * residues :, :lanes].astype(jnp.float32)
    bias_blocks = bias_blocks.reshape(sequences * H, lanes).astype(jnp.bfloat16)
    spread = one_hot(iota((lanes, lanes), 0) == iota((lanes, lanes), 1) % residues)
    bias_spread = dot_nn(bias_blocks, spread)
    own_head = iota(bias_spread.shape, 0) % H == iota(bias_spread.shape, 1) // residues
    bias_spread = jnp.where(own_head, bias_spread, 0.0).astype(jnp.bfloat16)
    from_place = iota((residues, sequences * H), 1) // H
    from_turn = from_place // subs
    from_dap = jnp.zeros_like(from_place)
    mask = 1
    while mask < daps:
        turned = from_turn // (daps // (2 * mask)) % 2
        kept = lax.rem(dap // mask, 2)
        from_dap = from_dap + mask * jnp.where(turned == 1, 1 - kept, kept)
        mask *= 2
    from_sub = sub - from_place % subs
    from_sub = jnp.where(from_sub < 0, from_sub + subs, from_sub)
    bias_order = one_hot(from_dap * subs + from_sub == iota(from_place.shape, 0))
    bias_rows = dot_nn(bias_order, bias_spread)
    turn = iota((tokens, tokens), 0)
    to_columns = one_hot(
        iota((tokens, tokens), 1) == (turn % sequences) * residues + turn // sequences
    )

    row_output = outputs_ref[: H * DH, :]
    column_output = outputs_ref[H * DH : 2 * H * DH, :]
    transition_out_at = 2 * H * DH

    row_weights = row_project_ref[...]
    values_in = alignment.astype(jnp.float32)
    normed_rows, scale_rows = normalize(values_in)
    normed_rows_low = normed_rows.astype(jnp.bfloat16)
    row_gated, row_saved = attend(normed_rows_low, row_weights, bias_rows, residues)
    after_rows = (values_in + dot_nn(row_gated, row_output)).astype(jnp.bfloat16)

    column_weights = column_project_ref[...]
    columns = dot_nn(to_columns, after_rows)
    upstream = dot_nn(to_columns, cotangent)
    upstream_low = upstream.astype(jnp.bfloat16)
    normed_cols, scale_cols = normalize(columns)
    normed_cols_low = normed_cols.astype(jnp.bfloat16)
    column_gated, column_saved = attend(normed_cols_low, column_weights, None, sequences)
    after_columns = (columns + dot_nn(column_gated, column_output)).astype(jnp.bfloat16)

    normed_two, scale_two = normalize(after_columns)
    normed_two_low = normed_two.astype(jnp.bfloat16)
    chosen_two = chosen(normed_two_low, C // sequences)
    unit_rows = hidden_units // sequences
    chunk = min(C, hidden_units)
    chosen_hidden = None
    grad_normed_two = None
    for at in range(0, hidden_units, chunk):
        gate_weight = transition_in_ref[:, at : at + chunk]
        up_weight = transition_in_ref[:, hidden_units + at : hidden_units + at + chunk]
        gate_part = dot_nn(normed_two_low, gate_weight)
        up_part = dot_nn(normed_two_low, up_weight)
        transition_out = outputs_ref[transition_out_at + at : transition_out_at + at + chunk, :]
        grad_hidden = dot_nt(upstream_low, transition_out)
        sigmoid_gate = jax.nn.sigmoid(gate_part)
        activated = gate_part * sigmoid_gate
        hidden = (activated * up_part).astype(jnp.bfloat16)
        grad_gate_part = (
            grad_hidden * up_part * sigmoid_gate * (1.0 + gate_part * (1.0 - sigmoid_gate))
        ).astype(jnp.bfloat16)
        grad_up_part = (grad_hidden * activated).astype(jnp.bfloat16)
        shape = (unit_rows, chunk)
        picked = one_hot(iota(shape, 1) + at == iota(shape, 0) + own * unit_rows)
        part = dot_nt(picked, hidden)
        chosen_hidden = part if chosen_hidden is None else chosen_hidden + part
        part = dot_nt(grad_gate_part, gate_weight) + dot_nt(grad_up_part, up_weight)
        grad_normed_two = part if grad_normed_two is None else grad_normed_two + part
        grad_transition_in_ref[:, 0, at : at + chunk] = (
            dot_nn(chosen_two, grad_gate_part) * token_scale
        )
        grad_transition_in_ref[:, 1, at : at + chunk] = (
            dot_nn(chosen_two, grad_up_part) * token_scale
        )
    grad_transition_out_ref[...] = (
        dot_nn(chosen_hidden.astype(jnp.bfloat16), upstream_low) * token_scale
    )
    grad_after_columns = upstream + norm_back(normed_two, scale_two, grad_normed_two)

    grad_columns_low = grad_after_columns.astype(jnp.bfloat16)
    column_grad_proj, unused = attend_back(
        column_saved, grad_columns_low, column_output, sequences
    )
    grad_column_output_ref[...] = (
        dot_nn(chosen(column_gated, C // sequences), grad_columns_low) * token_scale
    )
    raw = dot_nn(chosen(normed_cols_low, C // sequences), column_grad_proj) * token_scale
    for at in range(4):
        grad_column_project_ref[:, at, :] = raw[:, at * C : (at + 1) * C]
    grad_normed_cols = dot_nt(column_grad_proj, column_weights)
    grad_turned = (
        grad_after_columns + norm_back(normed_cols, scale_cols, grad_normed_cols)
    ).astype(jnp.bfloat16)

    grad_after_rows = dot_tn(to_columns, grad_turned)
    grad_rows_low = grad_after_rows.astype(jnp.bfloat16)
    row_grad_proj, row_grad_scores = attend_back(
        row_saved, grad_rows_low, row_output, residues
    )
    grad_row_output_ref[...] = (
        dot_nn(chosen(row_gated, C // sequences), grad_rows_low) * token_scale
    )
    raw = dot_nn(chosen(normed_rows_low, C // sequences), row_grad_proj) * token_scale
    for at in range(4):
        grad_row_project_ref[:, at, :] = raw[:, at * C : (at + 1) * C]
    bias_total = sum(part_rows(row_grad_scores, residues)) * (residues * sequences ** (-0.5))
    bias_own = jnp.sum(
        jnp.where(iota(bias_total.shape, 0) == own, bias_total, 0.0), axis=0, keepdims=True
    )
    for at in range(H):
        grad_bias_ref[at : at + 1, 0, :] = bias_own[:, at * residues : (at + 1) * residues]
    grad_normed_rows = dot_nt(row_grad_proj[:residues], row_weights)
    grad_alignment_ref[0] = (
        grad_after_rows[:residues]
        + norm_back(normed_rows[:residues], scale_rows[:residues], grad_normed_rows)
    ).astype(jnp.bfloat16)


def sample_call(daps, subs, residues, sequences, hidden_units):
    rows = C // sequences
    out_shape = (
        jax.ShapeDtypeStruct((1, residues, C), jnp.bfloat16),
        jax.ShapeDtypeStruct((H, 1, residues), jnp.float32),
        jax.ShapeDtypeStruct((rows, 4, H * DH), jnp.float32),
        jax.ShapeDtypeStruct((rows, C), jnp.float32),
        jax.ShapeDtypeStruct((rows, 4, H * DH), jnp.float32),
        jax.ShapeDtypeStruct((rows, C), jnp.float32),
        jax.ShapeDtypeStruct((rows, 2, hidden_units), jnp.float32),
        jax.ShapeDtypeStruct((hidden_units // sequences, C), jnp.float32),
    )
    return pl.pallas_call(
        lambda *refs: sample_kernel(*refs, daps=daps, subs=subs, residues=residues),
        out_shape=out_shape,
        in_specs=[pl.BlockSpec(memory_space=pltpu.VMEM)] * 5,
        out_specs=tuple(pl.BlockSpec(memory_space=pltpu.VMEM) for _ in out_shape),
        compiler_params=pltpu.CompilerParams(vmem_limit_bytes=KERNEL_VMEM_BYTES),
        name="sample",
    )


def around(values, axis):
    size = lax.axis_size(axis)
    blocks = [values]
    for shift in range(1, size):
        pairs = [(source, (source + shift) % size) for source in range(size)]
        blocks.append(lax.ppermute(values, axis, pairs))
    return jnp.concatenate(blocks, axis=0)


def doubled(values, axis, mask):
    pairs = [(source, source ^ mask) for source in range(lax.axis_size(axis))]
    return jnp.concatenate([values, lax.ppermute(values, axis, pairs)], axis=0)


def gathered(
    alignment,
    pair_bias,
    row_project,
    row_output,
    column_project,
    column_output,
    transition_in,
    transition_out,
    cotangent,
):
    daps = lax.axis_size("dap")
    subs = lax.axis_size("sub")
    residues = alignment.shape[1]
    hidden_units = transition_out.shape[0]
    bias_heads = jnp.pad(jnp.swapaxes(pair_bias, 0, 1), ((0, 0), (0, 0), (0, C - residues)))
    block = jnp.concatenate([alignment, cotangent, bias_heads], axis=1)
    blocks = around(lax.optimization_barrier(block), "sub")
    weights = (
        row_project.reshape(C, 4 * H * DH),
        column_project.reshape(C, 4 * H * DH),
        transition_in.reshape(C, 2 * hidden_units),
        jnp.concatenate([row_output, column_output, transition_out], axis=0),
    )
    blocks, weights = lax.optimization_barrier((blocks, weights))
    mask = daps // 2
    while mask:
        blocks = doubled(blocks, "dap", mask)
        mask //= 2
    return sample_call(daps, subs, residues, daps * subs, hidden_units)(blocks, *weights)


def gathered_fits(alignment, transition_out):
    sequences = alignment.shape[0] * lax.axis_size("dap") * lax.axis_size("sub")
    residues = alignment.shape[1]
    hidden_bytes = sequences * residues * 2 * transition_out.shape[0] * 4
    lengths_fit = all(
        length >= 16 and length & (length - 1) == 0 and H * length <= C
        for length in (sequences, residues)
    )
    return (
        alignment.shape[0] == 1
        and lax.axis_size("dap") & (lax.axis_size("dap") - 1) == 0
        and sequences == residues
        and lengths_fit
        and hidden_bytes <= GATHERED_HIDDEN_BYTES
    )


def shards(alignment, *others):
    transition_out = others[-2]
    plan = gathered if gathered_fits(alignment, transition_out) else distributed
    return plan(alignment, *others)


def solution(mesh):
    in_specs = (
        P(("grp", "dap", "sub"), None, None),
        P(None, ("grp", "dap", "sub"), None),
        P(),
        P(),
        P(),
        P(),
        P(),
        P(),
        P(("grp", "dap", "sub"), None, None),
    )
    out_specs = (
        P(("grp", "dap", "sub"), None, None),
        P(None, ("grp", "dap", "sub"), None),
        P(("grp", "dap", "sub"), None, None),
        P(("grp", "dap", "sub"), None),
        P(("grp", "dap", "sub"), None, None),
        P(("grp", "dap", "sub"), None),
        P(("grp", "dap", "sub"), None, None),
        P(("grp", "dap", "sub"), None),
    )
    return jax.shard_map(shards, mesh=mesh, in_specs=in_specs, out_specs=out_specs, check_vma=False)
```

```python
import jax
import jax.numpy as jnp
from jax import lax
from jax.experimental import pallas as pl
from jax.experimental.pallas import tpu as pltpu
from jax.sharding import PartitionSpec as P

C = 256
H = 8
DH = 32


EPSILON = 1e-05


def product(pattern, former, latter):
    return jnp.einsum(pattern, former, latter, preferred_element_type=jnp.float32)


def normalize(values):
    values = values.astype(jnp.float32)
    centred = values - jnp.mean(values, axis=-1, keepdims=True)
    factor = lax.rsqrt(jnp.mean(centred * centred, axis=-1, keepdims=True) + EPSILON)
    return (centred * factor, factor)


def norm_back(normed, factor, upstream):
    mean_up = jnp.mean(upstream, axis=-1, keepdims=True)
    mean_cross = jnp.mean(upstream * normed, axis=-1, keepdims=True)
    return factor * (upstream - mean_up - normed * mean_cross)


def run_items(function, arrays, sequential):
    if sequential:
        return lax.map(lambda bundle: function(*bundle), arrays)
    return jax.vmap(function)(*arrays)


def head_shares(queries, key_rows, bias_head):
    scores = product("qd,kd->qk", queries, key_rows)
    if bias_head is not None:
        scores = scores + bias_head.astype(jnp.float32)
    row_top = jnp.max(scores, axis=-1, keepdims=True)
    powered = jnp.exp(scores - row_top)
    return powered / jnp.sum(powered, axis=-1, keepdims=True)


def head_forward(queries, key_rows, values, bias_head=None):
    shares = head_shares(queries, key_rows, bias_head)
    return product("qk,kd->qd", shares.astype(jnp.bfloat16), values)


def head_backward(queries, key_rows, values, grad_blend, bias_head=None):
    shares = head_shares(queries, key_rows, bias_head)
    shares_low = shares.astype(jnp.bfloat16)
    blended = product("qk,kd->qd", shares_low, values)
    grad_shares = product("qd,kd->qk", grad_blend, values)
    grad_values = product("qk,qd->kd", shares_low, grad_blend)
    centre = jnp.sum(shares * grad_shares, axis=-1, keepdims=True)
    grad_scores = shares * (grad_shares - centre)
    grad_low = grad_scores.astype(jnp.bfloat16)
    grad_queries = product("qk,kd->qd", grad_low, key_rows)
    grad_keys = product("qk,qd->kd", grad_low, queries)
    return (blended, grad_queries, grad_keys, grad_values, grad_scores)


def item_project(normed_item, weights):
    projected = product("lc,cfhd->fhld", normed_item, weights.reshape(C, 4, H, DH))
    queries = (projected[0] * DH ** (-0.5)).astype(jnp.bfloat16)
    key_rows = projected[1].astype(jnp.bfloat16)
    values = projected[2].astype(jnp.bfloat16)
    gating = jax.nn.sigmoid(projected[3])
    return (queries, key_rows, values, gating)


def forward_item(normed_item, weights, bias_table, head_loop):
    queries, key_rows, values, gating = item_project(normed_item, weights)
    if bias_table is None:
        head_args = (queries, key_rows, values)
    else:
        head_args = (queries, key_rows, values, bias_table)
    blended = run_items(head_forward, head_args, head_loop)
    return (blended * gating).astype(jnp.bfloat16)


def backward_item(normed_item, upstream_item, weights, out_weight, bias_table, head_loop):
    queries, key_rows, values, gating = item_project(normed_item, weights)
    grad_gated = product("lc,hdc->hld", upstream_item, out_weight.reshape(H, DH, C))
    grad_blend = (grad_gated * gating).astype(jnp.bfloat16)
    if bias_table is None:
        head_args = (queries, key_rows, values, grad_blend)
    else:
        head_args = (queries, key_rows, values, grad_blend, bias_table)
    blended, grad_queries, grad_keys, grad_values, grad_scores = run_items(
        head_backward, head_args, head_loop
    )
    grad_gate = grad_gated * blended * gating * (1.0 - gating)
    grad_proj = jnp.stack(
        [grad_queries * DH ** (-0.5), grad_keys, grad_values, grad_gate], axis=0
    ).astype(jnp.bfloat16)
    if bias_table is None:
        return (grad_proj, jnp.zeros((), jnp.float32))
    return (grad_proj, grad_scores)


def section_forward(normed_low, weights, bias_table, item_loop, head_loop):

    def single(normed_item):
        return forward_item(normed_item, weights, bias_table, head_loop)

    return run_items(single, (normed_low,), item_loop)


def section_backward(
    normed_low, upstream_low, weights, out_weight, bias_table, item_loop, head_loop
):

    def single(normed_item, upstream_item):
        return backward_item(normed_item, upstream_item, weights, out_weight, bias_table, head_loop)

    if bias_table is None:
        grad_proj, unused = run_items(single, (normed_low, upstream_low), item_loop)
        return (grad_proj, None)

    def accumulate(running, bundle):
        grad_proj, grad_scores = single(bundle[0], bundle[1])
        return (running + grad_scores, grad_proj)

    bias_total, grad_proj = lax.scan(
        accumulate, jnp.zeros(bias_table.shape, jnp.float32), (normed_low, upstream_low)
    )
    return (grad_proj, bias_total)


def column_block(columns, upstream, column_project, column_output, transition_in, transition_out):
    normed_cols, scale_cols = normalize(columns)
    normed_cols_low = normed_cols.astype(jnp.bfloat16)
    column_gated = section_forward(normed_cols_low, column_project, None, False, False)
    column_update = product("bhld,hdc->blc", column_gated, column_output.reshape(H, DH, C))
    after_columns = (columns.astype(jnp.float32) + column_update).astype(jnp.bfloat16)
    normed_two, scale_two = normalize(after_columns)
    normed_two_low = normed_two.astype(jnp.bfloat16)
    pre_hidden = product("blc,cfe->blfe", normed_two_low, transition_in)
    gate_part = pre_hidden[:, :, 0]
    up_part = pre_hidden[:, :, 1]
    sigmoid_gate = jax.nn.sigmoid(gate_part)
    activated = gate_part * sigmoid_gate
    hidden = (activated * up_part).astype(jnp.bfloat16)
    raw_trans_out = product("blf,blc->fc", hidden, upstream)
    grad_hidden = product("blc,fc->blf", upstream, transition_out)
    grad_gate_part = grad_hidden * up_part * sigmoid_gate * (1.0 + gate_part * (1.0 - sigmoid_gate))
    grad_up_part = grad_hidden * activated
    grad_pre = jnp.stack([grad_gate_part, grad_up_part], axis=2).astype(jnp.bfloat16)
    raw_trans_in = product("blc,blfe->cfe", normed_two_low, grad_pre)
    grad_normed_two = product("blfe,cfe->blc", grad_pre, transition_in)
    grad_after_columns = upstream.astype(jnp.float32) + norm_back(
        normed_two, scale_two, grad_normed_two
    )
    grad_columns_low = grad_after_columns.astype(jnp.bfloat16)
    grad_proj, unused = section_backward(
        normed_cols_low, grad_columns_low, column_project, column_output, None, False, False
    )
    raw_column_output = product("bhld,blc->hdc", column_gated, grad_columns_low).reshape(H * DH, C)
    raw_column_project = product("blc,bfhld->cfhd", normed_cols_low, grad_proj).reshape(
        C, 4, H * DH
    )
    grad_normed_cols = product("bfhld,cfhd->blc", grad_proj, column_project.reshape(C, 4, H, DH))
    grad_after_rows = (
        grad_after_columns + norm_back(normed_cols, scale_cols, grad_normed_cols)
    ).astype(jnp.bfloat16)
    return (grad_after_rows, raw_column_project, raw_column_output, raw_trans_in, raw_trans_out)


def row_block(
    normed_rows,
    scale_rows,
    normed_rows_low,
    row_gated,
    grad_after_rows,
    row_project,
    row_output,
    bias_table,
):
    grad_proj, bias_total = section_backward(
        normed_rows_low, grad_after_rows, row_project, row_output, bias_table, True, True
    )
    raw_row_output = product("bhld,blc->hdc", row_gated, grad_after_rows).reshape(H * DH, C)
    raw_row_project = product("blc,bfhld->cfhd", normed_rows_low, grad_proj).reshape(C, 4, H * DH)
    grad_normed_rows = product("bfhld,cfhd->blc", grad_proj, row_project.reshape(C, 4, H, DH))
    grad_alignment = (
        grad_after_rows.astype(jnp.float32) + norm_back(normed_rows, scale_rows, grad_normed_rows)
    ).astype(jnp.bfloat16)
    return (grad_alignment, raw_row_project, raw_row_output, bias_total)


def to_columns(arranged):
    moved = lax.all_to_all(arranged, ("dap", "sub"), split_axis=1, concat_axis=0, tiled=True)
    return moved


def to_rows(arranged):
    moved = lax.all_to_all(arranged, ("dap", "sub"), split_axis=0, concat_axis=1, tiled=True)
    return moved


def distributed(
    alignment,
    pair_bias,
    row_project,
    row_output,
    column_project,
    column_output,
    transition_in,
    transition_out,
    cotangent,
):
    bias_full = lax.all_gather(pair_bias, ("dap", "sub"), axis=1, tiled=True)
    upstream = jnp.swapaxes(to_columns(cotangent), 0, 1)
    normed_rows, scale_rows = normalize(alignment)
    normed_rows_low = normed_rows.astype(jnp.bfloat16)
    row_gated = section_forward(normed_rows_low, row_project, bias_full, True, True)
    row_update = product("bhld,hdc->blc", row_gated, row_output.reshape(H, DH, C))
    after_rows = (alignment.astype(jnp.float32) + row_update).astype(jnp.bfloat16)
    columns = jnp.swapaxes(to_columns(after_rows), 0, 1)
    grad_columns, raw_column_project, raw_column_output, raw_trans_in, raw_trans_out = column_block(
        columns, upstream, column_project, column_output, transition_in, transition_out
    )
    sequences = alignment.shape[0] * lax.axis_size("dap") * lax.axis_size("sub")
    residues = alignment.shape[1]
    token_scale = (sequences * residues) ** (-0.5)
    term_col_project = raw_column_project * token_scale
    term_col_output = raw_column_output * token_scale
    term_trans_in = raw_trans_in * token_scale
    term_trans_out = raw_trans_out * token_scale
    grad_after_rows = to_rows(jnp.swapaxes(grad_columns, 0, 1))
    grad_alignment, raw_row_project, raw_row_output, bias_total = row_block(
        normed_rows,
        scale_rows,
        normed_rows_low,
        row_gated,
        grad_after_rows,
        row_project,
        row_output,
        bias_full,
    )
    term_row_project = raw_row_project * token_scale
    term_row_output = raw_row_output * token_scale
    bias_term = bias_total * (residues * sequences ** (-0.5))
    grad_bias = lax.psum_scatter(bias_term, ("dap", "sub"), scatter_dimension=1, tiled=True)
    (
        grad_row_project,
        grad_row_output,
        grad_col_project,
        grad_col_output,
        grad_trans_in,
        grad_trans_out,
    ) = (
        lax.psum_scatter(term_row_project, ("dap", "sub"), scatter_dimension=0, tiled=True),
        lax.psum_scatter(term_row_output, ("dap", "sub"), scatter_dimension=0, tiled=True),
        lax.psum_scatter(term_col_project, ("dap", "sub"), scatter_dimension=0, tiled=True),
        lax.psum_scatter(term_col_output, ("dap", "sub"), scatter_dimension=0, tiled=True),
        lax.psum_scatter(term_trans_in, ("dap", "sub"), scatter_dimension=0, tiled=True),
        lax.psum_scatter(term_trans_out, ("dap", "sub"), scatter_dimension=0, tiled=True),
    )
    return (
        grad_alignment,
        grad_bias,
        grad_row_project,
        grad_row_output,
        grad_col_project,
        grad_col_output,
        grad_trans_in,
        grad_trans_out,
    )


GATHERED_HIDDEN_BYTES = 8 * 2**20
KERNEL_VMEM_BYTES = 24 * 2**20


def dot_nn(former, latter):
    return lax.dot_general(
        former, latter, (((1,), (0,)), ((), ())), preferred_element_type=jnp.float32
    )


def dot_nt(former, latter):
    return lax.dot_general(
        former, latter, (((1,), (1,)), ((), ())), preferred_element_type=jnp.float32
    )


def dot_tn(former, latter):
    return lax.dot_general(
        former, latter, (((0,), (0,)), ((), ())), preferred_element_type=jnp.float32
    )


def iota(shape, axis):
    return lax.broadcasted_iota(jnp.int32, shape, axis)


def one_hot(condition):
    return jnp.where(condition, 1.0, 0.0).astype(jnp.bfloat16)


def grouped(values, length):
    return values.reshape(values.shape[0] // length, length, values.shape[1])


def by_head(rows, length):
    tall = jnp.concatenate([rows] * H, axis=0)
    own = iota(tall.shape, 0) // length == iota(tall.shape, 1) // DH
    return jnp.where(own, tall, jnp.zeros_like(tall))


def from_heads(tall, length):
    head = iota((length, tall.shape[1]), 1) // DH
    kept = tall[:length]
    for at in range(1, H):
        kept = jnp.where(head == at, tall[at * length : (at + 1) * length], kept)
    return kept


def part_rows(values, length):
    return [values[at : at + length] for at in range(0, values.shape[0], length)]


def attend(normed_low, weights, bias_keys, length):
    projected = [dot_nn(normed_low, weights[:, at * C : (at + 1) * C]) for at in range(4)]
    queries = (projected[0] * DH ** (-0.5)).astype(jnp.bfloat16)
    key_rows = projected[1].astype(jnp.bfloat16)
    values = projected[2].astype(jnp.bfloat16)
    gating = jax.nn.sigmoid(projected[3])
    scores = jnp.concatenate(
        [
            dot_nt(key, by_head(query, length))
            for query, key in zip(part_rows(queries, length), part_rows(key_rows, length))
        ],
        axis=0,
    )
    scores = grouped(scores, length)
    if bias_keys is not None:
        scores = scores + bias_keys[None]
    powered = jnp.exp(scores - jnp.max(scores, axis=1, keepdims=True))
    shares = powered / jnp.sum(powered, axis=1, keepdims=True)
    shares = shares.reshape(normed_low.shape[0], H * length)
    shares_low = shares.astype(jnp.bfloat16)
    blended = jnp.concatenate(
        [
            from_heads(dot_tn(share, value), length)
            for share, value in zip(part_rows(shares_low, length), part_rows(values, length))
        ],
        axis=0,
    )
    gated = (blended * gating).astype(jnp.bfloat16)
    return gated, (queries, key_rows, values, gating, shares, shares_low, blended)


def attend_back(saved, upstream_low, out_weight, length):
    queries, key_rows, values, gating, shares, shares_low, blended = saved
    grad_gated = dot_nt(upstream_low, out_weight)
    grad_blend = (grad_gated * gating).astype(jnp.bfloat16)
    grad_shares = []
    grad_values = []
    for share, grad, value in zip(
        part_rows(shares_low, length), part_rows(grad_blend, length), part_rows(values, length)
    ):
        grad_spread = by_head(grad, length)
        grad_shares.append(dot_nt(value, grad_spread))
        grad_values.append(dot_nn(share, grad_spread))
    shares = grouped(shares, length)
    grad_shares = grouped(jnp.concatenate(grad_shares, axis=0), length)
    centre = jnp.sum(shares * grad_shares, axis=1, keepdims=True)
    grad_scores = (shares * (grad_shares - centre)).reshape(upstream_low.shape[0], H * length)
    grad_low = grad_scores.astype(jnp.bfloat16)
    grad_queries = []
    grad_keys = []
    for score, key, query in zip(
        part_rows(grad_low, length), part_rows(key_rows, length), part_rows(queries, length)
    ):
        grad_queries.append(from_heads(dot_tn(score, key), length))
        grad_keys.append(dot_nn(score, by_head(query, length)))
    grad_gate = grad_gated * blended * gating * (1.0 - gating)
    grad_proj = jnp.concatenate(
        [
            (jnp.concatenate(grad_queries, axis=0) * DH ** (-0.5)).astype(jnp.bfloat16),
            jnp.concatenate(grad_keys, axis=0).astype(jnp.bfloat16),
            jnp.concatenate(grad_values, axis=0).astype(jnp.bfloat16),
            grad_gate.astype(jnp.bfloat16),
        ],
        axis=1,
    )
    return grad_proj, grad_scores


def sample_kernel(
    gathered_ref,
    row_project_ref,
    column_project_ref,
    transition_in_ref,
    outputs_ref,
    grad_alignment_ref,
    grad_bias_ref,
    grad_row_project_ref,
    grad_row_output_ref,
    grad_column_project_ref,
    grad_column_output_ref,
    grad_transition_in_ref,
    grad_transition_out_ref,
    *,
    daps,
    subs,
    residues,
):
    sequences = gathered_ref.shape[0]
    tokens = sequences * residues
    hidden_units = transition_in_ref.shape[1] // 2
    token_scale = tokens ** (-0.5)
    dap = lax.axis_index("dap")
    sub = lax.axis_index("sub")
    own = dap * subs + sub

    def chosen(values, count):
        shape = (count, values.shape[1])
        picked = one_hot(iota(shape, 1) == iota(shape, 0) + own * count)
        return dot_nt(picked, values).astype(jnp.bfloat16)

    alignment = gathered_ref[:, :residues, :].reshape(tokens, C)
    cotangent = gathered_ref[:, residues : 2 * residues, :].reshape(tokens, C)
    lanes = H * residues
    bias_blocks = gathered_ref[:, 2 * residues :, :lanes].astype(jnp.float32)
    bias_blocks = bias_blocks.reshape(sequences * H, lanes).astype(jnp.bfloat16)
    block_at = iota((sequences * H, lanes), 0)
    from_place = block_at // H
    from_turn = from_place // subs
    from_dap = jnp.zeros_like(from_place)
    mask = 1
    while mask < daps:
        turned = from_turn // (daps // (2 * mask)) % 2
        kept = lax.rem(dap // mask, 2)
        from_dap = from_dap + mask * jnp.where(turned == 1, 1 - kept, kept)
        mask *= 2
    from_sub = sub - from_place % subs
    from_sub = jnp.where(from_sub < 0, from_sub + subs, from_sub)
    query_lane = iota(block_at.shape, 1)
    bias_order = one_hot(
        (from_dap * subs + from_sub == query_lane % residues)
        & (block_at % H == query_lane // residues)
    )
    bias_keys = dot_tn(bias_blocks, bias_order)[:residues]
    turn = iota((tokens, tokens), 0)
    to_columns = one_hot(
        iota((tokens, tokens), 1) == (turn % sequences) * residues + turn // sequences
    )

    row_output = outputs_ref[: H * DH, :]
    column_output = outputs_ref[H * DH : 2 * H * DH, :]
    transition_out_at = 2 * H * DH

    row_weights = row_project_ref[...]
    values_in = alignment.astype(jnp.float32)
    normed_rows, scale_rows = normalize(values_in)
    normed_rows_low = normed_rows.astype(jnp.bfloat16)
    row_gated, row_saved = attend(normed_rows_low, row_weights, bias_keys, residues)
    after_rows = (values_in + dot_nn(row_gated, row_output)).astype(jnp.bfloat16)

    column_weights = column_project_ref[...]
    columns = dot_nn(to_columns, after_rows)
    upstream = dot_nn(to_columns, cotangent)
    upstream_low = upstream.astype(jnp.bfloat16)
    normed_cols, scale_cols = normalize(columns)
    normed_cols_low = normed_cols.astype(jnp.bfloat16)
    column_gated, column_saved = attend(normed_cols_low, column_weights, None, sequences)
    after_columns = (columns + dot_nn(column_gated, column_output)).astype(jnp.bfloat16)

    normed_two, scale_two = normalize(after_columns)
    normed_two_low = normed_two.astype(jnp.bfloat16)
    chosen_two = chosen(normed_two_low, C // sequences)
    unit_rows = hidden_units // sequences
    chunk = min(C, hidden_units)
    chosen_hidden = None
    grad_normed_two = None
    for at in range(0, hidden_units, chunk):
        gate_weight = transition_in_ref[:, at : at + chunk]
        up_weight = transition_in_ref[:, hidden_units + at : hidden_units + at + chunk]
        gate_part = dot_nn(normed_two_low, gate_weight)
        up_part = dot_nn(normed_two_low, up_weight)
        transition_out = outputs_ref[transition_out_at + at : transition_out_at + at + chunk, :]
        grad_hidden = dot_nt(upstream_low, transition_out)
        sigmoid_gate = jax.nn.sigmoid(gate_part)
        activated = gate_part * sigmoid_gate
        hidden = (activated * up_part).astype(jnp.bfloat16)
        grad_gate_part = (
            grad_hidden * up_part * sigmoid_gate * (1.0 + gate_part * (1.0 - sigmoid_gate))
        ).astype(jnp.bfloat16)
        grad_up_part = (grad_hidden * activated).astype(jnp.bfloat16)
        shape = (unit_rows, chunk)
        picked = one_hot(iota(shape, 1) + at == iota(shape, 0) + own * unit_rows)
        part = dot_nt(picked, hidden)
        chosen_hidden = part if chosen_hidden is None else chosen_hidden + part
        part = dot_nt(grad_gate_part, gate_weight) + dot_nt(grad_up_part, up_weight)
        grad_normed_two = part if grad_normed_two is None else grad_normed_two + part
        grad_transition_in_ref[:, 0, at : at + chunk] = (
            dot_nn(chosen_two, grad_gate_part) * token_scale
        )
        grad_transition_in_ref[:, 1, at : at + chunk] = (
            dot_nn(chosen_two, grad_up_part) * token_scale
        )
    grad_transition_out_ref[...] = (
        dot_nn(chosen_hidden.astype(jnp.bfloat16), upstream_low) * token_scale
    )
    grad_after_columns = upstream + norm_back(normed_two, scale_two, grad_normed_two)

    grad_columns_low = grad_after_columns.astype(jnp.bfloat16)
    column_grad_proj, unused = attend_back(
        column_saved, grad_columns_low, column_output, sequences
    )
    grad_column_output_ref[...] = (
        dot_nn(chosen(column_gated, C // sequences), grad_columns_low) * token_scale
    )
    raw = dot_nn(chosen(normed_cols_low, C // sequences), column_grad_proj) * token_scale
    for at in range(4):
        grad_column_project_ref[:, at, :] = raw[:, at * C : (at + 1) * C]
    grad_normed_cols = dot_nt(column_grad_proj, column_weights)
    grad_turned = (
        grad_after_columns + norm_back(normed_cols, scale_cols, grad_normed_cols)
    ).astype(jnp.bfloat16)

    grad_after_rows = dot_tn(to_columns, grad_turned)
    grad_rows_low = grad_after_rows.astype(jnp.bfloat16)
    row_grad_proj, row_grad_scores = attend_back(
        row_saved, grad_rows_low, row_output, residues
    )
    grad_row_output_ref[...] = (
        dot_nn(chosen(row_gated, C // sequences), grad_rows_low) * token_scale
    )
    raw = dot_nn(chosen(normed_rows_low, C // sequences), row_grad_proj) * token_scale
    for at in range(4):
        grad_row_project_ref[:, at, :] = raw[:, at * C : (at + 1) * C]
    bias_total = sum(part_rows(row_grad_scores, residues)) * (residues * sequences ** (-0.5))
    bias_high = bias_total.astype(jnp.bfloat16)
    bias_rest = (bias_total - bias_high.astype(jnp.float32)).astype(jnp.bfloat16)
    shape = (H, lanes)
    own_query = one_hot(iota(shape, 1) == iota(shape, 0) * residues + own)
    bias_own = dot_nt(own_query, bias_high) + dot_nt(own_query, bias_rest)
    for at in range(H):
        grad_bias_ref[at : at + 1, 0, :] = bias_own[at : at + 1, :]
    grad_normed_rows = dot_nt(row_grad_proj[:residues], row_weights)
    grad_alignment_ref[0] = (
        grad_after_rows[:residues]
        + norm_back(normed_rows[:residues], scale_rows[:residues], grad_normed_rows)
    ).astype(jnp.bfloat16)


def sample_call(daps, subs, residues, sequences, hidden_units):
    rows = C // sequences
    out_shape = (
        jax.ShapeDtypeStruct((1, residues, C), jnp.bfloat16),
        jax.ShapeDtypeStruct((H, 1, residues), jnp.float32),
        jax.ShapeDtypeStruct((rows, 4, H * DH), jnp.float32),
        jax.ShapeDtypeStruct((rows, C), jnp.float32),
        jax.ShapeDtypeStruct((rows, 4, H * DH), jnp.float32),
        jax.ShapeDtypeStruct((rows, C), jnp.float32),
        jax.ShapeDtypeStruct((rows, 2, hidden_units), jnp.float32),
        jax.ShapeDtypeStruct((hidden_units // sequences, C), jnp.float32),
    )
    return pl.pallas_call(
        lambda *refs: sample_kernel(*refs, daps=daps, subs=subs, residues=residues),
        out_shape=out_shape,
        in_specs=[pl.BlockSpec(memory_space=pltpu.VMEM)] * 5,
        out_specs=tuple(pl.BlockSpec(memory_space=pltpu.VMEM) for _ in out_shape),
        compiler_params=pltpu.CompilerParams(vmem_limit_bytes=KERNEL_VMEM_BYTES),
        name="sample",
    )


def around(values, axis):
    size = lax.axis_size(axis)
    blocks = [values]
    for shift in range(1, size):
        pairs = [(source, (source + shift) % size) for source in range(size)]
        blocks.append(lax.ppermute(values, axis, pairs))
    return jnp.concatenate(blocks, axis=0)


def doubled(values, axis, mask):
    pairs = [(source, source ^ mask) for source in range(lax.axis_size(axis))]
    return jnp.concatenate([values, lax.ppermute(values, axis, pairs)], axis=0)


def gathered(
    alignment,
    pair_bias,
    row_project,
    row_output,
    column_project,
    column_output,
    transition_in,
    transition_out,
    cotangent,
):
    daps = lax.axis_size("dap")
    subs = lax.axis_size("sub")
    residues = alignment.shape[1]
    hidden_units = transition_out.shape[0]
    bias_heads = jnp.pad(jnp.swapaxes(pair_bias, 0, 1), ((0, 0), (0, 0), (0, C - residues)))
    block = jnp.concatenate([alignment, cotangent, bias_heads], axis=1)
    blocks = around(lax.optimization_barrier(block), "sub")
    weights = (
        row_project.reshape(C, 4 * H * DH),
        column_project.reshape(C, 4 * H * DH),
        transition_in.reshape(C, 2 * hidden_units),
        jnp.concatenate([row_output, column_output, transition_out], axis=0),
    )
    blocks, weights = lax.optimization_barrier((blocks, weights))
    mask = daps // 2
    while mask:
        blocks = doubled(blocks, "dap", mask)
        mask //= 2
    return sample_call(daps, subs, residues, daps * subs, hidden_units)(blocks, *weights)


def gathered_fits(alignment, transition_out):
    sequences = alignment.shape[0] * lax.axis_size("dap") * lax.axis_size("sub")
    residues = alignment.shape[1]
    hidden_bytes = sequences * residues * 2 * transition_out.shape[0] * 4
    lengths_fit = all(
        length >= 16 and length & (length - 1) == 0 and H * length <= C
        for length in (sequences, residues)
    )
    return (
        alignment.shape[0] == 1
        and lax.axis_size("dap") & (lax.axis_size("dap") - 1) == 0
        and sequences == residues
        and lengths_fit
        and hidden_bytes <= GATHERED_HIDDEN_BYTES
    )


def shards(alignment, *others):
    transition_out = others[-2]
    plan = gathered if gathered_fits(alignment, transition_out) else distributed
    return plan(alignment, *others)


def solution(mesh):
    in_specs = (
        P(("grp", "dap", "sub"), None, None),
        P(None, ("grp", "dap", "sub"), None),
        P(),
        P(),
        P(),
        P(),
        P(),
        P(),
        P(("grp", "dap", "sub"), None, None),
    )
    out_specs = (
        P(("grp", "dap", "sub"), None, None),
        P(None, ("grp", "dap", "sub"), None),
        P(("grp", "dap", "sub"), None, None),
        P(("grp", "dap", "sub"), None),
        P(("grp", "dap", "sub"), None, None),
        P(("grp", "dap", "sub"), None),
        P(("grp", "dap", "sub"), None, None),
        P(("grp", "dap", "sub"), None),
    )
    return jax.shard_map(shards, mesh=mesh, in_specs=in_specs, out_specs=out_specs, check_vma=False)
```

```python
import jax
import jax.numpy as jnp
from jax import lax
from jax.experimental import pallas as pl
from jax.experimental.pallas import tpu as pltpu
from jax.sharding import PartitionSpec as P

C = 256
H = 8
DH = 32


EPSILON = 1e-05


def product(pattern, former, latter):
    return jnp.einsum(pattern, former, latter, preferred_element_type=jnp.float32)


def normalize(values):
    values = values.astype(jnp.float32)
    centred = values - jnp.mean(values, axis=-1, keepdims=True)
    factor = lax.rsqrt(jnp.mean(centred * centred, axis=-1, keepdims=True) + EPSILON)
    return (centred * factor, factor)


def norm_back(normed, factor, upstream):
    mean_up = jnp.mean(upstream, axis=-1, keepdims=True)
    mean_cross = jnp.mean(upstream * normed, axis=-1, keepdims=True)
    return factor * (upstream - mean_up - normed * mean_cross)


def run_items(function, arrays, sequential):
    if sequential:
        return lax.map(lambda bundle: function(*bundle), arrays)
    return jax.vmap(function)(*arrays)


def head_shares(queries, key_rows, bias_head):
    scores = product("qd,kd->qk", queries, key_rows)
    if bias_head is not None:
        scores = scores + bias_head.astype(jnp.float32)
    row_top = jnp.max(scores, axis=-1, keepdims=True)
    powered = jnp.exp(scores - row_top)
    return powered / jnp.sum(powered, axis=-1, keepdims=True)


def head_forward(queries, key_rows, values, bias_head=None):
    shares = head_shares(queries, key_rows, bias_head)
    return product("qk,kd->qd", shares.astype(jnp.bfloat16), values)


def head_backward(queries, key_rows, values, grad_blend, bias_head=None):
    shares = head_shares(queries, key_rows, bias_head)
    shares_low = shares.astype(jnp.bfloat16)
    blended = product("qk,kd->qd", shares_low, values)
    grad_shares = product("qd,kd->qk", grad_blend, values)
    grad_values = product("qk,qd->kd", shares_low, grad_blend)
    centre = jnp.sum(shares * grad_shares, axis=-1, keepdims=True)
    grad_scores = shares * (grad_shares - centre)
    grad_low = grad_scores.astype(jnp.bfloat16)
    grad_queries = product("qk,kd->qd", grad_low, key_rows)
    grad_keys = product("qk,qd->kd", grad_low, queries)
    return (blended, grad_queries, grad_keys, grad_values, grad_scores)


def item_project(normed_item, weights):
    projected = product("lc,cfhd->fhld", normed_item, weights.reshape(C, 4, H, DH))
    queries = (projected[0] * DH ** (-0.5)).astype(jnp.bfloat16)
    key_rows = projected[1].astype(jnp.bfloat16)
    values = projected[2].astype(jnp.bfloat16)
    gating = jax.nn.sigmoid(projected[3])
    return (queries, key_rows, values, gating)


def forward_item(normed_item, weights, bias_table, head_loop):
    queries, key_rows, values, gating = item_project(normed_item, weights)
    if bias_table is None:
        head_args = (queries, key_rows, values)
    else:
        head_args = (queries, key_rows, values, bias_table)
    blended = run_items(head_forward, head_args, head_loop)
    return (blended * gating).astype(jnp.bfloat16)


def backward_item(normed_item, upstream_item, weights, out_weight, bias_table, head_loop):
    queries, key_rows, values, gating = item_project(normed_item, weights)
    grad_gated = product("lc,hdc->hld", upstream_item, out_weight.reshape(H, DH, C))
    grad_blend = (grad_gated * gating).astype(jnp.bfloat16)
    if bias_table is None:
        head_args = (queries, key_rows, values, grad_blend)
    else:
        head_args = (queries, key_rows, values, grad_blend, bias_table)
    blended, grad_queries, grad_keys, grad_values, grad_scores = run_items(
        head_backward, head_args, head_loop
    )
    grad_gate = grad_gated * blended * gating * (1.0 - gating)
    grad_proj = jnp.stack(
        [grad_queries * DH ** (-0.5), grad_keys, grad_values, grad_gate], axis=0
    ).astype(jnp.bfloat16)
    if bias_table is None:
        return (grad_proj, jnp.zeros((), jnp.float32))
    return (grad_proj, grad_scores)


def section_forward(normed_low, weights, bias_table, item_loop, head_loop):

    def single(normed_item):
        return forward_item(normed_item, weights, bias_table, head_loop)

    return run_items(single, (normed_low,), item_loop)


def section_backward(
    normed_low, upstream_low, weights, out_weight, bias_table, item_loop, head_loop
):

    def single(normed_item, upstream_item):
        return backward_item(normed_item, upstream_item, weights, out_weight, bias_table, head_loop)

    if bias_table is None:
        grad_proj, unused = run_items(single, (normed_low, upstream_low), item_loop)
        return (grad_proj, None)

    def accumulate(running, bundle):
        grad_proj, grad_scores = single(bundle[0], bundle[1])
        return (running + grad_scores, grad_proj)

    bias_total, grad_proj = lax.scan(
        accumulate, jnp.zeros(bias_table.shape, jnp.float32), (normed_low, upstream_low)
    )
    return (grad_proj, bias_total)


def column_block(columns, upstream, column_project, column_output, transition_in, transition_out):
    normed_cols, scale_cols = normalize(columns)
    normed_cols_low = normed_cols.astype(jnp.bfloat16)
    column_gated = section_forward(normed_cols_low, column_project, None, False, False)
    column_update = product("bhld,hdc->blc", column_gated, column_output.reshape(H, DH, C))
    after_columns = (columns.astype(jnp.float32) + column_update).astype(jnp.bfloat16)
    normed_two, scale_two = normalize(after_columns)
    normed_two_low = normed_two.astype(jnp.bfloat16)
    pre_hidden = product("blc,cfe->blfe", normed_two_low, transition_in)
    gate_part = pre_hidden[:, :, 0]
    up_part = pre_hidden[:, :, 1]
    sigmoid_gate = jax.nn.sigmoid(gate_part)
    activated = gate_part * sigmoid_gate
    hidden = (activated * up_part).astype(jnp.bfloat16)
    raw_trans_out = product("blf,blc->fc", hidden, upstream)
    grad_hidden = product("blc,fc->blf", upstream, transition_out)
    grad_gate_part = grad_hidden * up_part * sigmoid_gate * (1.0 + gate_part * (1.0 - sigmoid_gate))
    grad_up_part = grad_hidden * activated
    grad_pre = jnp.stack([grad_gate_part, grad_up_part], axis=2).astype(jnp.bfloat16)
    raw_trans_in = product("blc,blfe->cfe", normed_two_low, grad_pre)
    grad_normed_two = product("blfe,cfe->blc", grad_pre, transition_in)
    grad_after_columns = upstream.astype(jnp.float32) + norm_back(
        normed_two, scale_two, grad_normed_two
    )
    grad_columns_low = grad_after_columns.astype(jnp.bfloat16)
    grad_proj, unused = section_backward(
        normed_cols_low, grad_columns_low, column_project, column_output, None, False, False
    )
    raw_column_output = product("bhld,blc->hdc", column_gated, grad_columns_low).reshape(H * DH, C)
    raw_column_project = product("blc,bfhld->cfhd", normed_cols_low, grad_proj).reshape(
        C, 4, H * DH
    )
    grad_normed_cols = product("bfhld,cfhd->blc", grad_proj, column_project.reshape(C, 4, H, DH))
    grad_after_rows = (
        grad_after_columns + norm_back(normed_cols, scale_cols, grad_normed_cols)
    ).astype(jnp.bfloat16)
    return (grad_after_rows, raw_column_project, raw_column_output, raw_trans_in, raw_trans_out)


def row_block(
    normed_rows,
    scale_rows,
    normed_rows_low,
    row_gated,
    grad_after_rows,
    row_project,
    row_output,
    bias_table,
):
    grad_proj, bias_total = section_backward(
        normed_rows_low, grad_after_rows, row_project, row_output, bias_table, True, True
    )
    raw_row_output = product("bhld,blc->hdc", row_gated, grad_after_rows).reshape(H * DH, C)
    raw_row_project = product("blc,bfhld->cfhd", normed_rows_low, grad_proj).reshape(C, 4, H * DH)
    grad_normed_rows = product("bfhld,cfhd->blc", grad_proj, row_project.reshape(C, 4, H, DH))
    grad_alignment = (
        grad_after_rows.astype(jnp.float32) + norm_back(normed_rows, scale_rows, grad_normed_rows)
    ).astype(jnp.bfloat16)
    return (grad_alignment, raw_row_project, raw_row_output, bias_total)


def to_columns(arranged):
    moved = lax.all_to_all(arranged, ("dap", "sub"), split_axis=1, concat_axis=0, tiled=True)
    return moved


def to_rows(arranged):
    moved = lax.all_to_all(arranged, ("dap", "sub"), split_axis=0, concat_axis=1, tiled=True)
    return moved


def distributed(
    alignment,
    pair_bias,
    row_project,
    row_output,
    column_project,
    column_output,
    transition_in,
    transition_out,
    cotangent,
):
    bias_full = lax.all_gather(pair_bias, ("dap", "sub"), axis=1, tiled=True)
    upstream = jnp.swapaxes(to_columns(cotangent), 0, 1)
    normed_rows, scale_rows = normalize(alignment)
    normed_rows_low = normed_rows.astype(jnp.bfloat16)
    row_gated = section_forward(normed_rows_low, row_project, bias_full, True, True)
    row_update = product("bhld,hdc->blc", row_gated, row_output.reshape(H, DH, C))
    after_rows = (alignment.astype(jnp.float32) + row_update).astype(jnp.bfloat16)
    columns = jnp.swapaxes(to_columns(after_rows), 0, 1)
    grad_columns, raw_column_project, raw_column_output, raw_trans_in, raw_trans_out = column_block(
        columns, upstream, column_project, column_output, transition_in, transition_out
    )
    sequences = alignment.shape[0] * lax.axis_size("dap") * lax.axis_size("sub")
    residues = alignment.shape[1]
    token_scale = (sequences * residues) ** (-0.5)
    term_col_project = raw_column_project * token_scale
    term_col_output = raw_column_output * token_scale
    term_trans_in = raw_trans_in * token_scale
    term_trans_out = raw_trans_out * token_scale
    grad_after_rows = to_rows(jnp.swapaxes(grad_columns, 0, 1))
    grad_alignment, raw_row_project, raw_row_output, bias_total = row_block(
        normed_rows,
        scale_rows,
        normed_rows_low,
        row_gated,
        grad_after_rows,
        row_project,
        row_output,
        bias_full,
    )
    term_row_project = raw_row_project * token_scale
    term_row_output = raw_row_output * token_scale
    bias_term = bias_total * (residues * sequences ** (-0.5))
    grad_bias = lax.psum_scatter(bias_term, ("dap", "sub"), scatter_dimension=1, tiled=True)
    (
        grad_row_project,
        grad_row_output,
        grad_col_project,
        grad_col_output,
        grad_trans_in,
        grad_trans_out,
    ) = (
        lax.psum_scatter(term_row_project, ("dap", "sub"), scatter_dimension=0, tiled=True),
        lax.psum_scatter(term_row_output, ("dap", "sub"), scatter_dimension=0, tiled=True),
        lax.psum_scatter(term_col_project, ("dap", "sub"), scatter_dimension=0, tiled=True),
        lax.psum_scatter(term_col_output, ("dap", "sub"), scatter_dimension=0, tiled=True),
        lax.psum_scatter(term_trans_in, ("dap", "sub"), scatter_dimension=0, tiled=True),
        lax.psum_scatter(term_trans_out, ("dap", "sub"), scatter_dimension=0, tiled=True),
    )
    return (
        grad_alignment,
        grad_bias,
        grad_row_project,
        grad_row_output,
        grad_col_project,
        grad_col_output,
        grad_trans_in,
        grad_trans_out,
    )


GATHERED_HIDDEN_BYTES = 8 * 2**20
KERNEL_VMEM_BYTES = 24 * 2**20


def dot_nn(former, latter):
    return lax.dot_general(
        former, latter, (((1,), (0,)), ((), ())), preferred_element_type=jnp.float32
    )


def dot_nt(former, latter):
    return lax.dot_general(
        former, latter, (((1,), (1,)), ((), ())), preferred_element_type=jnp.float32
    )


def dot_tn(former, latter):
    return lax.dot_general(
        former, latter, (((0,), (0,)), ((), ())), preferred_element_type=jnp.float32
    )


def iota(shape, axis):
    return lax.broadcasted_iota(jnp.int32, shape, axis)


def one_hot(condition):
    return jnp.where(condition, 1.0, 0.0).astype(jnp.bfloat16)


def grouped(values, length):
    return values.reshape(values.shape[0] // length, length, values.shape[1])


def part_of(values, size):
    return lax.shift_right_logical(values, jnp.full_like(values, size.bit_length() - 1))


def place_in(values, size):
    return values & (size - 1)


LANES = 128
TILE_HEADS = LANES // DH


def by_head(rows, length):
    head = part_of(iota((length, LANES), 1), DH)
    none = jnp.zeros((length, LANES), rows.dtype)
    tall = []
    for at in range(H):
        own = at // TILE_HEADS
        tile = rows[:, own * LANES : (own + 1) * LANES]
        tile = jnp.where(head == at % TILE_HEADS, tile, none)
        tiles = [tile if other == own else none for other in range(H // TILE_HEADS)]
        tall.append(jnp.concatenate(tiles, axis=1))
    return jnp.concatenate(tall, axis=0)


def turned_product(former, latter, length):
    turned = jnp.transpose(former)
    head = part_of(iota((length, LANES), 1), DH)
    tiles = []
    for at in range(H // TILE_HEADS):
        rows = turned[at * TILE_HEADS * length : (at + 1) * TILE_HEADS * length]
        tall = dot_nn(rows, latter[:, at * LANES : (at + 1) * LANES])
        kept = tall[:length]
        for other in range(1, TILE_HEADS):
            kept = jnp.where(head == other, tall[other * length : (other + 1) * length], kept)
        tiles.append(kept)
    return jnp.concatenate(tiles, axis=1)


def part_rows(values, length):
    return [values[at : at + length] for at in range(0, values.shape[0], length)]


def attend(normed_low, weights, bias_keys, length):
    projected = [dot_nn(normed_low, weights[:, at * C : (at + 1) * C]) for at in range(4)]
    queries = (projected[0] * DH ** (-0.5)).astype(jnp.bfloat16)
    key_rows = projected[1].astype(jnp.bfloat16)
    values = projected[2].astype(jnp.bfloat16)
    gating = jax.nn.sigmoid(projected[3])
    scores = jnp.concatenate(
        [
            dot_nt(key, by_head(query, length))
            for query, key in zip(part_rows(queries, length), part_rows(key_rows, length))
        ],
        axis=0,
    )
    scores = grouped(scores, length)
    if bias_keys is not None:
        scores = scores + bias_keys[None]
    powered = jnp.exp(scores - jnp.max(scores, axis=1, keepdims=True))
    shares = powered / jnp.sum(powered, axis=1, keepdims=True)
    shares = shares.reshape(normed_low.shape[0], H * length)
    shares_low = shares.astype(jnp.bfloat16)
    blended = jnp.concatenate(
        [
            turned_product(share, value, length)
            for share, value in zip(part_rows(shares_low, length), part_rows(values, length))
        ],
        axis=0,
    )
    gated = (blended * gating).astype(jnp.bfloat16)
    return gated, (queries, key_rows, values, gating, shares, shares_low, blended)


def attend_back(saved, upstream_low, out_weight, length):
    queries, key_rows, values, gating, shares, shares_low, blended = saved
    grad_gated = dot_nt(upstream_low, out_weight)
    grad_blend = (grad_gated * gating).astype(jnp.bfloat16)
    grad_shares = []
    grad_values = []
    for share, grad, value in zip(
        part_rows(shares_low, length), part_rows(grad_blend, length), part_rows(values, length)
    ):
        grad_spread = by_head(grad, length)
        grad_shares.append(dot_nt(value, grad_spread))
        grad_values.append(dot_nn(share, grad_spread))
    shares = grouped(shares, length)
    grad_shares = grouped(jnp.concatenate(grad_shares, axis=0), length)
    centre = jnp.sum(shares * grad_shares, axis=1, keepdims=True)
    grad_scores = (shares * (grad_shares - centre)).reshape(upstream_low.shape[0], H * length)
    grad_low = grad_scores.astype(jnp.bfloat16)
    grad_queries = []
    grad_keys = []
    for score, key, query in zip(
        part_rows(grad_low, length), part_rows(key_rows, length), part_rows(queries, length)
    ):
        grad_queries.append(turned_product(score, key, length))
        grad_keys.append(dot_nn(score, by_head(query, length)))
    grad_gate = grad_gated * blended * gating * (1.0 - gating)
    grad_proj = jnp.concatenate(
        [
            (jnp.concatenate(grad_queries, axis=0) * DH ** (-0.5)).astype(jnp.bfloat16),
            jnp.concatenate(grad_keys, axis=0).astype(jnp.bfloat16),
            jnp.concatenate(grad_values, axis=0).astype(jnp.bfloat16),
            grad_gate.astype(jnp.bfloat16),
        ],
        axis=1,
    )
    return grad_proj, grad_scores


def sample_kernel(
    gathered_ref,
    row_project_ref,
    column_project_ref,
    transition_in_ref,
    outputs_ref,
    grad_alignment_ref,
    grad_bias_ref,
    grad_row_project_ref,
    grad_row_output_ref,
    grad_column_project_ref,
    grad_column_output_ref,
    grad_transition_in_ref,
    grad_transition_out_ref,
    *,
    daps,
    subs,
    residues,
):
    sequences = gathered_ref.shape[0]
    tokens = sequences * residues
    hidden_units = transition_in_ref.shape[1] // 2
    token_scale = tokens ** (-0.5)
    dap = lax.axis_index("dap")
    sub = lax.axis_index("sub")
    own = dap * subs + sub

    def chosen(values, count):
        shape = (count, values.shape[1])
        picked = one_hot(iota(shape, 1) == iota(shape, 0) + own * count)
        return dot_nt(picked, values).astype(jnp.bfloat16)

    alignment = gathered_ref[:, :residues, :].reshape(tokens, C)
    cotangent = gathered_ref[:, residues : 2 * residues, :].reshape(tokens, C)
    lanes = H * residues
    bias_blocks = gathered_ref[:, 2 * residues :, :lanes].astype(jnp.float32)
    bias_blocks = bias_blocks.reshape(sequences * H, lanes).astype(jnp.bfloat16)
    block_at = iota((sequences * H, lanes), 0)
    from_place = part_of(block_at, H)
    from_turn = part_of(from_place, subs)
    from_dap = jnp.zeros_like(from_place)
    mask = 1
    while mask < daps:
        turned = place_in(part_of(from_turn, daps // (2 * mask)), 2)
        kept = lax.rem(dap // mask, 2)
        from_dap = from_dap + mask * jnp.where(turned == 1, 1 - kept, kept)
        mask *= 2
    from_sub = place_in(sub + from_place, subs)
    query_lane = iota(block_at.shape, 1)
    bias_order = one_hot(
        (from_dap * subs + from_sub == place_in(query_lane, residues))
        & (place_in(block_at, H) == part_of(query_lane, residues))
    )
    bias_keys = dot_tn(bias_blocks, bias_order)[:residues]
    turn = iota((tokens, tokens), 0)
    to_columns = one_hot(
        iota((tokens, tokens), 1) == place_in(turn, sequences) * residues + part_of(turn, sequences)
    )

    row_output = outputs_ref[: H * DH, :]
    column_output = outputs_ref[H * DH : 2 * H * DH, :]
    transition_out_at = 2 * H * DH

    row_weights = row_project_ref[...]
    values_in = alignment.astype(jnp.float32)
    normed_rows, scale_rows = normalize(values_in)
    normed_rows_low = normed_rows.astype(jnp.bfloat16)
    row_gated, row_saved = attend(normed_rows_low, row_weights, bias_keys, residues)
    after_rows = (values_in + dot_nn(row_gated, row_output)).astype(jnp.bfloat16)

    column_weights = column_project_ref[...]
    columns = dot_nn(to_columns, after_rows)
    upstream = dot_nn(to_columns, cotangent)
    upstream_low = upstream.astype(jnp.bfloat16)
    normed_cols, scale_cols = normalize(columns)
    normed_cols_low = normed_cols.astype(jnp.bfloat16)
    column_gated, column_saved = attend(normed_cols_low, column_weights, None, sequences)
    after_columns = (columns + dot_nn(column_gated, column_output)).astype(jnp.bfloat16)

    normed_two, scale_two = normalize(after_columns)
    normed_two_low = normed_two.astype(jnp.bfloat16)
    chosen_two = chosen(normed_two_low, C // sequences)
    unit_rows = hidden_units // sequences
    chunk = min(C, hidden_units)
    chosen_hidden = None
    grad_normed_two = None
    for at in range(0, hidden_units, chunk):
        gate_weight = transition_in_ref[:, at : at + chunk]
        up_weight = transition_in_ref[:, hidden_units + at : hidden_units + at + chunk]
        gate_part = dot_nn(normed_two_low, gate_weight)
        up_part = dot_nn(normed_two_low, up_weight)
        transition_out = outputs_ref[transition_out_at + at : transition_out_at + at + chunk, :]
        grad_hidden = dot_nt(upstream_low, transition_out)
        sigmoid_gate = jax.nn.sigmoid(gate_part)
        activated = gate_part * sigmoid_gate
        hidden = (activated * up_part).astype(jnp.bfloat16)
        grad_gate_part = (
            grad_hidden * up_part * sigmoid_gate * (1.0 + gate_part * (1.0 - sigmoid_gate))
        ).astype(jnp.bfloat16)
        grad_up_part = (grad_hidden * activated).astype(jnp.bfloat16)
        shape = (unit_rows, chunk)
        picked = one_hot(iota(shape, 1) + at == iota(shape, 0) + own * unit_rows)
        part = dot_nt(picked, hidden)
        chosen_hidden = part if chosen_hidden is None else chosen_hidden + part
        part = dot_nt(grad_gate_part, gate_weight) + dot_nt(grad_up_part, up_weight)
        grad_normed_two = part if grad_normed_two is None else grad_normed_two + part
        grad_transition_in_ref[:, 0, at : at + chunk] = (
            dot_nn(chosen_two, grad_gate_part) * token_scale
        )
        grad_transition_in_ref[:, 1, at : at + chunk] = (
            dot_nn(chosen_two, grad_up_part) * token_scale
        )
    grad_transition_out_ref[...] = (
        dot_nn(chosen_hidden.astype(jnp.bfloat16), upstream_low) * token_scale
    )
    grad_after_columns = upstream + norm_back(normed_two, scale_two, grad_normed_two)

    grad_columns_low = grad_after_columns.astype(jnp.bfloat16)
    column_grad_proj, unused = attend_back(
        column_saved, grad_columns_low, column_output, sequences
    )
    grad_column_output_ref[...] = (
        dot_nn(chosen(column_gated, C // sequences), grad_columns_low) * token_scale
    )
    raw = dot_nn(chosen(normed_cols_low, C // sequences), column_grad_proj) * token_scale
    for at in range(4):
        grad_column_project_ref[:, at, :] = raw[:, at * C : (at + 1) * C]
    grad_normed_cols = dot_nt(column_grad_proj, column_weights)
    grad_turned = (
        grad_after_columns + norm_back(normed_cols, scale_cols, grad_normed_cols)
    ).astype(jnp.bfloat16)

    grad_after_rows = dot_tn(to_columns, grad_turned)
    grad_rows_low = grad_after_rows.astype(jnp.bfloat16)
    row_grad_proj, row_grad_scores = attend_back(
        row_saved, grad_rows_low, row_output, residues
    )
    grad_row_output_ref[...] = (
        dot_nn(chosen(row_gated, C // sequences), grad_rows_low) * token_scale
    )
    raw = dot_nn(chosen(normed_rows_low, C // sequences), row_grad_proj) * token_scale
    for at in range(4):
        grad_row_project_ref[:, at, :] = raw[:, at * C : (at + 1) * C]
    bias_total = sum(part_rows(row_grad_scores, residues)) * (residues * sequences ** (-0.5))
    bias_high = bias_total.astype(jnp.bfloat16)
    bias_rest = (bias_total - bias_high.astype(jnp.float32)).astype(jnp.bfloat16)
    shape = (H, lanes)
    own_query = one_hot(iota(shape, 1) == iota(shape, 0) * residues + own)
    bias_own = dot_nt(own_query, bias_high) + dot_nt(own_query, bias_rest)
    for at in range(H):
        grad_bias_ref[at : at + 1, 0, :] = bias_own[at : at + 1, :]
    grad_normed_rows = dot_nt(row_grad_proj[:residues], row_weights)
    grad_alignment_ref[0] = (
        grad_after_rows[:residues]
        + norm_back(normed_rows[:residues], scale_rows[:residues], grad_normed_rows)
    ).astype(jnp.bfloat16)


def sample_call(daps, subs, residues, sequences, hidden_units):
    rows = C // sequences
    out_shape = (
        jax.ShapeDtypeStruct((1, residues, C), jnp.bfloat16),
        jax.ShapeDtypeStruct((H, 1, residues), jnp.float32),
        jax.ShapeDtypeStruct((rows, 4, H * DH), jnp.float32),
        jax.ShapeDtypeStruct((rows, C), jnp.float32),
        jax.ShapeDtypeStruct((rows, 4, H * DH), jnp.float32),
        jax.ShapeDtypeStruct((rows, C), jnp.float32),
        jax.ShapeDtypeStruct((rows, 2, hidden_units), jnp.float32),
        jax.ShapeDtypeStruct((hidden_units // sequences, C), jnp.float32),
    )
    return pl.pallas_call(
        lambda *refs: sample_kernel(*refs, daps=daps, subs=subs, residues=residues),
        out_shape=out_shape,
        in_specs=[pl.BlockSpec(memory_space=pltpu.VMEM)] * 5,
        out_specs=tuple(pl.BlockSpec(memory_space=pltpu.VMEM) for _ in out_shape),
        compiler_params=pltpu.CompilerParams(vmem_limit_bytes=KERNEL_VMEM_BYTES),
        name="sample",
    )


def around(values, axis):
    size = lax.axis_size(axis)
    blocks = [values]
    for shift in range(1, size):
        pairs = [(source, (source - shift) % size) for source in range(size)]
        blocks.append(lax.ppermute(values, axis, pairs))
    return jnp.concatenate(blocks, axis=0)


def doubled(values, axis, mask):
    pairs = [(source, source ^ mask) for source in range(lax.axis_size(axis))]
    return jnp.concatenate([values, lax.ppermute(values, axis, pairs)], axis=0)


def gathered(
    alignment,
    pair_bias,
    row_project,
    row_output,
    column_project,
    column_output,
    transition_in,
    transition_out,
    cotangent,
):
    daps = lax.axis_size("dap")
    subs = lax.axis_size("sub")
    residues = alignment.shape[1]
    hidden_units = transition_out.shape[0]
    bias_heads = jnp.pad(jnp.swapaxes(pair_bias, 0, 1), ((0, 0), (0, 0), (0, C - residues)))
    block = jnp.concatenate([alignment, cotangent, bias_heads], axis=1)
    blocks = around(lax.optimization_barrier(block), "sub")
    weights = (
        row_project.reshape(C, 4 * H * DH),
        column_project.reshape(C, 4 * H * DH),
        transition_in.reshape(C, 2 * hidden_units),
        jnp.concatenate([row_output, column_output, transition_out], axis=0),
    )
    blocks, weights = lax.optimization_barrier((blocks, weights))
    mask = daps // 2
    while mask:
        blocks = doubled(blocks, "dap", mask)
        mask //= 2
    return sample_call(daps, subs, residues, daps * subs, hidden_units)(blocks, *weights)


def gathered_fits(alignment, transition_out):
    sequences = alignment.shape[0] * lax.axis_size("dap") * lax.axis_size("sub")
    residues = alignment.shape[1]
    hidden_bytes = sequences * residues * 2 * transition_out.shape[0] * 4
    lengths_fit = all(
        length >= 16 and length & (length - 1) == 0 and H * length <= C
        for length in (sequences, residues)
    )
    return (
        alignment.shape[0] == 1
        and lax.axis_size("dap") & (lax.axis_size("dap") - 1) == 0
        and sequences == residues
        and lengths_fit
        and hidden_bytes <= GATHERED_HIDDEN_BYTES
    )


def shards(alignment, *others):
    transition_out = others[-2]
    plan = gathered if gathered_fits(alignment, transition_out) else distributed
    return plan(alignment, *others)


def solution(mesh):
    in_specs = (
        P(("grp", "dap", "sub"), None, None),
        P(None, ("grp", "dap", "sub"), None),
        P(),
        P(),
        P(),
        P(),
        P(),
        P(),
        P(("grp", "dap", "sub"), None, None),
    )
    out_specs = (
        P(("grp", "dap", "sub"), None, None),
        P(None, ("grp", "dap", "sub"), None),
        P(("grp", "dap", "sub"), None, None),
        P(("grp", "dap", "sub"), None),
        P(("grp", "dap", "sub"), None, None),
        P(("grp", "dap", "sub"), None),
        P(("grp", "dap", "sub"), None, None),
        P(("grp", "dap", "sub"), None),
    )
    return jax.shard_map(shards, mesh=mesh, in_specs=in_specs, out_specs=out_specs, check_vma=False)
```

```python
import jax
import jax.numpy as jnp
from jax import lax
from jax.experimental import pallas as pl
from jax.experimental.pallas import tpu as pltpu
from jax.sharding import PartitionSpec as P

C = 256
H = 8
DH = 32


EPSILON = 1e-05


def product(pattern, former, latter):
    return jnp.einsum(pattern, former, latter, preferred_element_type=jnp.float32)


def normalize(values):
    values = values.astype(jnp.float32)
    centred = values - jnp.mean(values, axis=-1, keepdims=True)
    factor = lax.rsqrt(jnp.mean(centred * centred, axis=-1, keepdims=True) + EPSILON)
    return (centred * factor, factor)


def norm_back(normed, factor, upstream):
    mean_up = jnp.mean(upstream, axis=-1, keepdims=True)
    mean_cross = jnp.mean(upstream * normed, axis=-1, keepdims=True)
    return factor * (upstream - mean_up - normed * mean_cross)


def run_items(function, arrays, sequential):
    if sequential:
        return lax.map(lambda bundle: function(*bundle), arrays)
    return jax.vmap(function)(*arrays)


def head_shares(queries, key_rows, bias_head):
    scores = product("qd,kd->qk", queries, key_rows)
    if bias_head is not None:
        scores = scores + bias_head.astype(jnp.float32)
    row_top = jnp.max(scores, axis=-1, keepdims=True)
    powered = jnp.exp(scores - row_top)
    return powered / jnp.sum(powered, axis=-1, keepdims=True)


def head_forward(queries, key_rows, values, bias_head=None):
    shares = head_shares(queries, key_rows, bias_head)
    return product("qk,kd->qd", shares.astype(jnp.bfloat16), values)


def head_backward(queries, key_rows, values, grad_blend, bias_head=None):
    shares = head_shares(queries, key_rows, bias_head)
    shares_low = shares.astype(jnp.bfloat16)
    blended = product("qk,kd->qd", shares_low, values)
    grad_shares = product("qd,kd->qk", grad_blend, values)
    grad_values = product("qk,qd->kd", shares_low, grad_blend)
    centre = jnp.sum(shares * grad_shares, axis=-1, keepdims=True)
    grad_scores = shares * (grad_shares - centre)
    grad_low = grad_scores.astype(jnp.bfloat16)
    grad_queries = product("qk,kd->qd", grad_low, key_rows)
    grad_keys = product("qk,qd->kd", grad_low, queries)
    return (blended, grad_queries, grad_keys, grad_values, grad_scores)


def item_project(normed_item, weights):
    projected = product("lc,cfhd->fhld", normed_item, weights.reshape(C, 4, H, DH))
    queries = (projected[0] * DH ** (-0.5)).astype(jnp.bfloat16)
    key_rows = projected[1].astype(jnp.bfloat16)
    values = projected[2].astype(jnp.bfloat16)
    gating = jax.nn.sigmoid(projected[3])
    return (queries, key_rows, values, gating)


def forward_item(normed_item, weights, bias_table, head_loop):
    queries, key_rows, values, gating = item_project(normed_item, weights)
    if bias_table is None:
        head_args = (queries, key_rows, values)
    else:
        head_args = (queries, key_rows, values, bias_table)
    blended = run_items(head_forward, head_args, head_loop)
    return (blended * gating).astype(jnp.bfloat16)


def backward_item(normed_item, upstream_item, weights, out_weight, bias_table, head_loop):
    queries, key_rows, values, gating = item_project(normed_item, weights)
    grad_gated = product("lc,hdc->hld", upstream_item, out_weight.reshape(H, DH, C))
    grad_blend = (grad_gated * gating).astype(jnp.bfloat16)
    if bias_table is None:
        head_args = (queries, key_rows, values, grad_blend)
    else:
        head_args = (queries, key_rows, values, grad_blend, bias_table)
    blended, grad_queries, grad_keys, grad_values, grad_scores = run_items(
        head_backward, head_args, head_loop
    )
    grad_gate = grad_gated * blended * gating * (1.0 - gating)
    grad_proj = jnp.stack(
        [grad_queries * DH ** (-0.5), grad_keys, grad_values, grad_gate], axis=0
    ).astype(jnp.bfloat16)
    if bias_table is None:
        return (grad_proj, jnp.zeros((), jnp.float32))
    return (grad_proj, grad_scores)


def section_forward(normed_low, weights, bias_table, item_loop, head_loop):

    def single(normed_item):
        return forward_item(normed_item, weights, bias_table, head_loop)

    return run_items(single, (normed_low,), item_loop)


def section_backward(
    normed_low, upstream_low, weights, out_weight, bias_table, item_loop, head_loop
):

    def single(normed_item, upstream_item):
        return backward_item(normed_item, upstream_item, weights, out_weight, bias_table, head_loop)

    if bias_table is None:
        grad_proj, unused = run_items(single, (normed_low, upstream_low), item_loop)
        return (grad_proj, None)

    def accumulate(running, bundle):
        grad_proj, grad_scores = single(bundle[0], bundle[1])
        return (running + grad_scores, grad_proj)

    bias_total, grad_proj = lax.scan(
        accumulate, jnp.zeros(bias_table.shape, jnp.float32), (normed_low, upstream_low)
    )
    return (grad_proj, bias_total)


def column_block(columns, upstream, column_project, column_output, transition_in, transition_out):
    normed_cols, scale_cols = normalize(columns)
    normed_cols_low = normed_cols.astype(jnp.bfloat16)
    column_gated = section_forward(normed_cols_low, column_project, None, False, False)
    column_update = product("bhld,hdc->blc", column_gated, column_output.reshape(H, DH, C))
    after_columns = (columns.astype(jnp.float32) + column_update).astype(jnp.bfloat16)
    normed_two, scale_two = normalize(after_columns)
    normed_two_low = normed_two.astype(jnp.bfloat16)
    pre_hidden = product("blc,cfe->blfe", normed_two_low, transition_in)
    gate_part = pre_hidden[:, :, 0]
    up_part = pre_hidden[:, :, 1]
    sigmoid_gate = jax.nn.sigmoid(gate_part)
    activated = gate_part * sigmoid_gate
    hidden = (activated * up_part).astype(jnp.bfloat16)
    raw_trans_out = product("blf,blc->fc", hidden, upstream)
    grad_hidden = product("blc,fc->blf", upstream, transition_out)
    grad_gate_part = grad_hidden * up_part * sigmoid_gate * (1.0 + gate_part * (1.0 - sigmoid_gate))
    grad_up_part = grad_hidden * activated
    grad_pre = jnp.stack([grad_gate_part, grad_up_part], axis=2).astype(jnp.bfloat16)
    raw_trans_in = product("blc,blfe->cfe", normed_two_low, grad_pre)
    grad_normed_two = product("blfe,cfe->blc", grad_pre, transition_in)
    grad_after_columns = upstream.astype(jnp.float32) + norm_back(
        normed_two, scale_two, grad_normed_two
    )
    grad_columns_low = grad_after_columns.astype(jnp.bfloat16)
    grad_proj, unused = section_backward(
        normed_cols_low, grad_columns_low, column_project, column_output, None, False, False
    )
    raw_column_output = product("bhld,blc->hdc", column_gated, grad_columns_low).reshape(H * DH, C)
    raw_column_project = product("blc,bfhld->cfhd", normed_cols_low, grad_proj).reshape(
        C, 4, H * DH
    )
    grad_normed_cols = product("bfhld,cfhd->blc", grad_proj, column_project.reshape(C, 4, H, DH))
    grad_after_rows = (
        grad_after_columns + norm_back(normed_cols, scale_cols, grad_normed_cols)
    ).astype(jnp.bfloat16)
    return (grad_after_rows, raw_column_project, raw_column_output, raw_trans_in, raw_trans_out)


def row_block(
    normed_rows,
    scale_rows,
    normed_rows_low,
    row_gated,
    grad_after_rows,
    row_project,
    row_output,
    bias_table,
):
    grad_proj, bias_total = section_backward(
        normed_rows_low, grad_after_rows, row_project, row_output, bias_table, True, True
    )
    raw_row_output = product("bhld,blc->hdc", row_gated, grad_after_rows).reshape(H * DH, C)
    raw_row_project = product("blc,bfhld->cfhd", normed_rows_low, grad_proj).reshape(C, 4, H * DH)
    grad_normed_rows = product("bfhld,cfhd->blc", grad_proj, row_project.reshape(C, 4, H, DH))
    grad_alignment = (
        grad_after_rows.astype(jnp.float32) + norm_back(normed_rows, scale_rows, grad_normed_rows)
    ).astype(jnp.bfloat16)
    return (grad_alignment, raw_row_project, raw_row_output, bias_total)


def to_columns(arranged):
    moved = lax.all_to_all(arranged, ("dap", "sub"), split_axis=1, concat_axis=0, tiled=True)
    return moved


def to_rows(arranged):
    moved = lax.all_to_all(arranged, ("dap", "sub"), split_axis=0, concat_axis=1, tiled=True)
    return moved


def distributed(
    alignment,
    pair_bias,
    row_project,
    row_output,
    column_project,
    column_output,
    transition_in,
    transition_out,
    cotangent,
):
    bias_full = lax.all_gather(pair_bias, ("dap", "sub"), axis=1, tiled=True)
    upstream = jnp.swapaxes(to_columns(cotangent), 0, 1)
    normed_rows, scale_rows = normalize(alignment)
    normed_rows_low = normed_rows.astype(jnp.bfloat16)
    row_gated = section_forward(normed_rows_low, row_project, bias_full, True, True)
    row_update = product("bhld,hdc->blc", row_gated, row_output.reshape(H, DH, C))
    after_rows = (alignment.astype(jnp.float32) + row_update).astype(jnp.bfloat16)
    columns = jnp.swapaxes(to_columns(after_rows), 0, 1)
    grad_columns, raw_column_project, raw_column_output, raw_trans_in, raw_trans_out = column_block(
        columns, upstream, column_project, column_output, transition_in, transition_out
    )
    sequences = alignment.shape[0] * lax.axis_size("dap") * lax.axis_size("sub")
    residues = alignment.shape[1]
    token_scale = (sequences * residues) ** (-0.5)
    term_col_project = raw_column_project * token_scale
    term_col_output = raw_column_output * token_scale
    term_trans_in = raw_trans_in * token_scale
    term_trans_out = raw_trans_out * token_scale
    grad_after_rows = to_rows(jnp.swapaxes(grad_columns, 0, 1))
    grad_alignment, raw_row_project, raw_row_output, bias_total = row_block(
        normed_rows,
        scale_rows,
        normed_rows_low,
        row_gated,
        grad_after_rows,
        row_project,
        row_output,
        bias_full,
    )
    term_row_project = raw_row_project * token_scale
    term_row_output = raw_row_output * token_scale
    bias_term = bias_total * (residues * sequences ** (-0.5))
    grad_bias = lax.psum_scatter(bias_term, ("dap", "sub"), scatter_dimension=1, tiled=True)
    (
        grad_row_project,
        grad_row_output,
        grad_col_project,
        grad_col_output,
        grad_trans_in,
        grad_trans_out,
    ) = (
        lax.psum_scatter(term_row_project, ("dap", "sub"), scatter_dimension=0, tiled=True),
        lax.psum_scatter(term_row_output, ("dap", "sub"), scatter_dimension=0, tiled=True),
        lax.psum_scatter(term_col_project, ("dap", "sub"), scatter_dimension=0, tiled=True),
        lax.psum_scatter(term_col_output, ("dap", "sub"), scatter_dimension=0, tiled=True),
        lax.psum_scatter(term_trans_in, ("dap", "sub"), scatter_dimension=0, tiled=True),
        lax.psum_scatter(term_trans_out, ("dap", "sub"), scatter_dimension=0, tiled=True),
    )
    return (
        grad_alignment,
        grad_bias,
        grad_row_project,
        grad_row_output,
        grad_col_project,
        grad_col_output,
        grad_trans_in,
        grad_trans_out,
    )


GATHERED_HIDDEN_BYTES = 8 * 2**20
KERNEL_VMEM_BYTES = 24 * 2**20


def dot_nn(former, latter):
    return lax.dot_general(
        former, latter, (((1,), (0,)), ((), ())), preferred_element_type=jnp.float32
    )


def dot_nt(former, latter):
    return lax.dot_general(
        former, latter, (((1,), (1,)), ((), ())), preferred_element_type=jnp.float32
    )


def dot_tn(former, latter):
    return lax.dot_general(
        former, latter, (((0,), (0,)), ((), ())), preferred_element_type=jnp.float32
    )


def iota(shape, axis):
    return lax.broadcasted_iota(jnp.int32, shape, axis)


def one_hot(condition):
    return jnp.where(condition, 1.0, 0.0).astype(jnp.bfloat16)


def grouped(values, length):
    return values.reshape(values.shape[0] // length, length, values.shape[1])


def part_of(values, size):
    return lax.shift_right_logical(values, jnp.full_like(values, size.bit_length() - 1))


def place_in(values, size):
    return values & (size - 1)


LANES = 128
TILE_HEADS = LANES // DH


def by_head(rows, length):
    head = part_of(iota((length, LANES), 1), DH)
    none = jnp.zeros((length, LANES), rows.dtype)
    tall = []
    for at in range(H):
        own = at // TILE_HEADS
        tile = rows[:, own * LANES : (own + 1) * LANES]
        tile = jnp.where(head == at % TILE_HEADS, tile, none)
        tiles = [tile if other == own else none for other in range(H // TILE_HEADS)]
        tall.append(jnp.concatenate(tiles, axis=1))
    return jnp.concatenate(tall, axis=0)


def turned_product(former, latter, length):
    turned = jnp.transpose(former)
    head = part_of(iota((length, LANES), 1), DH)
    tiles = []
    for at in range(H // TILE_HEADS):
        rows = turned[at * TILE_HEADS * length : (at + 1) * TILE_HEADS * length]
        tall = dot_nn(rows, latter[:, at * LANES : (at + 1) * LANES])
        kept = tall[:length]
        for other in range(1, TILE_HEADS):
            kept = jnp.where(head == other, tall[other * length : (other + 1) * length], kept)
        tiles.append(kept)
    return jnp.concatenate(tiles, axis=1)


def part_rows(values, length):
    return [values[at : at + length] for at in range(0, values.shape[0], length)]


def attend(normed_low, weights, bias_keys, length):
    projected = [dot_nn(normed_low, weights[:, at * C : (at + 1) * C]) for at in range(4)]
    queries = (projected[0] * DH ** (-0.5)).astype(jnp.bfloat16)
    key_rows = projected[1].astype(jnp.bfloat16)
    values = projected[2].astype(jnp.bfloat16)
    gating = jax.nn.sigmoid(projected[3])
    scores = jnp.concatenate(
        [
            dot_nt(key, by_head(query, length))
            for query, key in zip(part_rows(queries, length), part_rows(key_rows, length))
        ],
        axis=0,
    )
    scores = grouped(scores, length)
    if bias_keys is not None:
        scores = scores + bias_keys[None]
    powered = jnp.exp(scores - jnp.max(scores, axis=1, keepdims=True))
    shares = powered / jnp.sum(powered, axis=1, keepdims=True)
    shares = shares.reshape(normed_low.shape[0], H * length)
    shares_low = shares.astype(jnp.bfloat16)
    blended = jnp.concatenate(
        [
            turned_product(share, value, length)
            for share, value in zip(part_rows(shares_low, length), part_rows(values, length))
        ],
        axis=0,
    )
    gated = (blended * gating).astype(jnp.bfloat16)
    return gated, (queries, key_rows, values, gating, shares, shares_low, blended)


def attend_back(saved, upstream_low, out_weight, length):
    queries, key_rows, values, gating, shares, shares_low, blended = saved
    grad_gated = dot_nt(upstream_low, out_weight)
    grad_blend = (grad_gated * gating).astype(jnp.bfloat16)
    grad_shares = []
    grad_values = []
    for share, grad, value in zip(
        part_rows(shares_low, length), part_rows(grad_blend, length), part_rows(values, length)
    ):
        grad_spread = by_head(grad, length)
        grad_shares.append(dot_nt(value, grad_spread))
        grad_values.append(dot_nn(share, grad_spread))
    shares = grouped(shares, length)
    grad_shares = grouped(jnp.concatenate(grad_shares, axis=0), length)
    centre = jnp.sum(shares * grad_shares, axis=1, keepdims=True)
    grad_scores = (shares * (grad_shares - centre)).reshape(upstream_low.shape[0], H * length)
    grad_low = grad_scores.astype(jnp.bfloat16)
    grad_queries = []
    grad_keys = []
    for score, key, query in zip(
        part_rows(grad_low, length), part_rows(key_rows, length), part_rows(queries, length)
    ):
        grad_queries.append(turned_product(score, key, length))
        grad_keys.append(dot_nn(score, by_head(query, length)))
    grad_gate = grad_gated * blended * gating * (1.0 - gating)
    grad_proj = jnp.concatenate(
        [
            (jnp.concatenate(grad_queries, axis=0) * DH ** (-0.5)).astype(jnp.bfloat16),
            jnp.concatenate(grad_keys, axis=0).astype(jnp.bfloat16),
            jnp.concatenate(grad_values, axis=0).astype(jnp.bfloat16),
            grad_gate.astype(jnp.bfloat16),
        ],
        axis=1,
    )
    return grad_proj, grad_scores


def sample_kernel(
    gathered_ref,
    row_project_ref,
    column_project_ref,
    transition_in_ref,
    outputs_ref,
    grad_alignment_ref,
    grad_bias_ref,
    grad_row_project_ref,
    grad_row_output_ref,
    grad_column_project_ref,
    grad_column_output_ref,
    grad_transition_in_ref,
    grad_transition_out_ref,
    *,
    daps,
    subs,
    residues,
):
    sequences = gathered_ref.shape[0]
    tokens = sequences * residues
    hidden_units = transition_in_ref.shape[1] // 2
    token_scale = tokens ** (-0.5)
    dap = lax.axis_index("dap")
    sub = lax.axis_index("sub")
    own = dap * subs + sub

    def chosen(values, count):
        shape = (count, values.shape[1])
        picked = one_hot(iota(shape, 1) == iota(shape, 0) + own * count)
        return dot_nt(picked, values).astype(jnp.bfloat16)

    alignment = gathered_ref[:, :residues, :].reshape(tokens, C)
    cotangent = gathered_ref[:, residues : 2 * residues, :].reshape(tokens, C)
    lanes = H * residues
    bias_blocks = gathered_ref[:, 2 * residues :, :lanes].astype(jnp.float32)
    bias_blocks = bias_blocks.reshape(sequences * H, lanes).astype(jnp.bfloat16)
    block_at = iota((sequences * H, lanes), 0)
    from_place = part_of(block_at, H)
    from_turn = part_of(from_place, subs)
    from_dap = jnp.zeros_like(from_place)
    mask = 1
    while mask < daps:
        turned = place_in(part_of(from_turn, daps // (2 * mask)), 2)
        kept = lax.rem(dap // mask, 2)
        from_dap = from_dap + mask * jnp.where(turned == 1, 1 - kept, kept)
        mask *= 2
    from_sub = place_in(sub + from_place, subs)
    query_lane = iota(block_at.shape, 1)
    bias_order = one_hot(
        (from_dap * subs + from_sub == place_in(query_lane, residues))
        & (place_in(block_at, H) == part_of(query_lane, residues))
    )
    bias_keys = dot_tn(bias_blocks, bias_order)[:residues]
    turn = iota((tokens, tokens), 0)
    to_columns = one_hot(
        iota((tokens, tokens), 1) == place_in(turn, sequences) * residues + part_of(turn, sequences)
    )

    row_output = outputs_ref[: H * DH, :]
    column_output = outputs_ref[H * DH : 2 * H * DH, :]
    transition_out_at = 2 * H * DH

    row_weights = row_project_ref[...]
    values_in = alignment.astype(jnp.float32)
    normed_rows, scale_rows = normalize(values_in)
    normed_rows_low = normed_rows.astype(jnp.bfloat16)
    row_gated, row_saved = attend(normed_rows_low, row_weights, bias_keys, residues)
    after_rows = (values_in + dot_nn(row_gated, row_output)).astype(jnp.bfloat16)

    column_weights = column_project_ref[...]
    columns = dot_nn(to_columns, after_rows)
    upstream = dot_nn(to_columns, cotangent)
    upstream_low = upstream.astype(jnp.bfloat16)
    normed_cols, scale_cols = normalize(columns)
    normed_cols_low = normed_cols.astype(jnp.bfloat16)
    column_gated, column_saved = attend(normed_cols_low, column_weights, None, sequences)
    after_columns = (columns + dot_nn(column_gated, column_output)).astype(jnp.bfloat16)

    normed_two, scale_two = normalize(after_columns)
    normed_two_low = normed_two.astype(jnp.bfloat16)
    chosen_two = chosen(normed_two_low, C // sequences)
    unit_rows = hidden_units // sequences
    chunk = min(C, hidden_units)
    chosen_hidden = None
    grad_normed_two = None
    for at in range(0, hidden_units, chunk):
        gate_weight = transition_in_ref[:, at : at + chunk]
        up_weight = transition_in_ref[:, hidden_units + at : hidden_units + at + chunk]
        gate_part = dot_nn(normed_two_low, gate_weight)
        up_part = dot_nn(normed_two_low, up_weight)
        transition_out = outputs_ref[transition_out_at + at : transition_out_at + at + chunk, :]
        grad_hidden = dot_nt(upstream_low, transition_out)
        sigmoid_gate = jax.nn.sigmoid(gate_part)
        activated = gate_part * sigmoid_gate
        hidden = (activated * up_part).astype(jnp.bfloat16)
        grad_gate_part = (
            grad_hidden * up_part * sigmoid_gate * (1.0 + gate_part * (1.0 - sigmoid_gate))
        ).astype(jnp.bfloat16)
        grad_up_part = (grad_hidden * activated).astype(jnp.bfloat16)
        shape = (unit_rows, chunk)
        picked = one_hot(iota(shape, 1) + at == iota(shape, 0) + own * unit_rows)
        part = dot_nt(picked, hidden)
        chosen_hidden = part if chosen_hidden is None else chosen_hidden + part
        part = dot_nt(grad_gate_part, gate_weight) + dot_nt(grad_up_part, up_weight)
        grad_normed_two = part if grad_normed_two is None else grad_normed_two + part
        grad_transition_in_ref[:, 0, at : at + chunk] = (
            dot_nn(chosen_two, grad_gate_part) * token_scale
        )
        grad_transition_in_ref[:, 1, at : at + chunk] = (
            dot_nn(chosen_two, grad_up_part) * token_scale
        )
    grad_transition_out_ref[...] = (
        dot_nn(chosen_hidden.astype(jnp.bfloat16), upstream_low) * token_scale
    )
    grad_after_columns = upstream + norm_back(normed_two, scale_two, grad_normed_two)

    grad_columns_low = grad_after_columns.astype(jnp.bfloat16)
    column_grad_proj, unused = attend_back(
        column_saved, grad_columns_low, column_output, sequences
    )
    grad_column_output_ref[...] = (
        dot_nn(chosen(column_gated, C // sequences), grad_columns_low) * token_scale
    )
    raw = dot_nn(chosen(normed_cols_low, C // sequences), column_grad_proj) * token_scale
    for at in range(4):
        grad_column_project_ref[:, at, :] = raw[:, at * C : (at + 1) * C]
    grad_normed_cols = dot_nt(column_grad_proj, column_weights)
    grad_turned = (
        grad_after_columns + norm_back(normed_cols, scale_cols, grad_normed_cols)
    ).astype(jnp.bfloat16)

    grad_after_rows = dot_tn(to_columns, grad_turned)
    grad_rows_low = grad_after_rows.astype(jnp.bfloat16)
    row_grad_proj, row_grad_scores = attend_back(
        row_saved, grad_rows_low, row_output, residues
    )
    grad_row_output_ref[...] = (
        dot_nn(chosen(row_gated, C // sequences), grad_rows_low) * token_scale
    )
    raw = dot_nn(chosen(normed_rows_low, C // sequences), row_grad_proj) * token_scale
    for at in range(4):
        grad_row_project_ref[:, at, :] = raw[:, at * C : (at + 1) * C]
    bias_total = sum(part_rows(row_grad_scores, residues)) * (residues * sequences ** (-0.5))
    bias_high = bias_total.astype(jnp.bfloat16)
    bias_rest = (bias_total - bias_high.astype(jnp.float32)).astype(jnp.bfloat16)
    shape = (H, lanes)
    own_query = one_hot(iota(shape, 1) == iota(shape, 0) * residues + own)
    bias_own = dot_nt(own_query, bias_high) + dot_nt(own_query, bias_rest)
    for at in range(H):
        grad_bias_ref[at : at + 1, 0, :] = bias_own[at : at + 1, :]
    grad_normed_rows = dot_nt(row_grad_proj[:residues], row_weights)
    grad_alignment_ref[0] = (
        grad_after_rows[:residues]
        + norm_back(normed_rows[:residues], scale_rows[:residues], grad_normed_rows)
    ).astype(jnp.bfloat16)


def sample_call(daps, subs, residues, sequences, hidden_units):
    rows = C // sequences
    out_shape = (
        jax.ShapeDtypeStruct((1, residues, C), jnp.bfloat16),
        jax.ShapeDtypeStruct((H, 1, residues), jnp.float32),
        jax.ShapeDtypeStruct((rows, 4, H * DH), jnp.float32),
        jax.ShapeDtypeStruct((rows, C), jnp.float32),
        jax.ShapeDtypeStruct((rows, 4, H * DH), jnp.float32),
        jax.ShapeDtypeStruct((rows, C), jnp.float32),
        jax.ShapeDtypeStruct((rows, 2, hidden_units), jnp.float32),
        jax.ShapeDtypeStruct((hidden_units // sequences, C), jnp.float32),
    )
    return pl.pallas_call(
        lambda *refs: sample_kernel(*refs, daps=daps, subs=subs, residues=residues),
        out_shape=out_shape,
        in_specs=[pl.BlockSpec(memory_space=pltpu.VMEM)] * 5,
        out_specs=tuple(pl.BlockSpec(memory_space=pltpu.VMEM) for _ in out_shape),
        compiler_params=pltpu.CompilerParams(vmem_limit_bytes=KERNEL_VMEM_BYTES),
        name="sample",
    )


def around(values, axis):
    size = lax.axis_size(axis)
    blocks = [values]
    for shift in range(1, size):
        pairs = [(source, (source - shift) % size) for source in range(size)]
        blocks.append(lax.ppermute(values, axis, pairs))
    return jnp.concatenate(blocks, axis=0)


def doubled(values, axis, mask):
    pairs = [(source, source ^ mask) for source in range(lax.axis_size(axis))]
    return jnp.concatenate([values, lax.ppermute(values, axis, pairs)], axis=0)


def gathered(
    alignment,
    pair_bias,
    row_project,
    row_output,
    column_project,
    column_output,
    transition_in,
    transition_out,
    cotangent,
):
    daps = lax.axis_size("dap")
    subs = lax.axis_size("sub")
    residues = alignment.shape[1]
    hidden_units = transition_out.shape[0]
    bias_heads = jnp.pad(jnp.swapaxes(pair_bias, 0, 1), ((0, 0), (0, 0), (0, C - residues)))
    block = jnp.concatenate([alignment, cotangent, bias_heads], axis=1)
    blocks = around(lax.optimization_barrier(block), "sub")
    early = (row_project.reshape(C, 4 * H * DH), column_project.reshape(C, 4 * H * DH))
    late = (
        transition_in.reshape(C, 2 * hidden_units),
        jnp.concatenate([row_output, column_output, transition_out], axis=0),
    )
    blocks, early = lax.optimization_barrier((blocks, early))
    mask = daps // 2
    while mask:
        blocks = doubled(blocks, "dap", mask)
        if mask > 1:
            blocks, late = lax.optimization_barrier((blocks, late))
        mask //= 2
    return sample_call(daps, subs, residues, daps * subs, hidden_units)(blocks, *early, *late)


def gathered_fits(alignment, transition_out):
    sequences = alignment.shape[0] * lax.axis_size("dap") * lax.axis_size("sub")
    residues = alignment.shape[1]
    hidden_bytes = sequences * residues * 2 * transition_out.shape[0] * 4
    lengths_fit = all(
        length >= 16 and length & (length - 1) == 0 and H * length <= C
        for length in (sequences, residues)
    )
    return (
        alignment.shape[0] == 1
        and lax.axis_size("dap") & (lax.axis_size("dap") - 1) == 0
        and sequences == residues
        and lengths_fit
        and hidden_bytes <= GATHERED_HIDDEN_BYTES
    )


def shards(alignment, *others):
    transition_out = others[-2]
    plan = gathered if gathered_fits(alignment, transition_out) else distributed
    return plan(alignment, *others)


def solution(mesh):
    in_specs = (
        P(("grp", "dap", "sub"), None, None),
        P(None, ("grp", "dap", "sub"), None),
        P(),
        P(),
        P(),
        P(),
        P(),
        P(),
        P(("grp", "dap", "sub"), None, None),
    )
    out_specs = (
        P(("grp", "dap", "sub"), None, None),
        P(None, ("grp", "dap", "sub"), None),
        P(("grp", "dap", "sub"), None, None),
        P(("grp", "dap", "sub"), None),
        P(("grp", "dap", "sub"), None, None),
        P(("grp", "dap", "sub"), None),
        P(("grp", "dap", "sub"), None, None),
        P(("grp", "dap", "sub"), None),
    )
    return jax.shard_map(shards, mesh=mesh, in_specs=in_specs, out_specs=out_specs, check_vma=False)
```
